32 devices in a mesh: dp: 8 (over z, y), mp: 4 (over x, core).
Axes of the slice: x: 2, y: 2, z: 4, core: 2. Of those that a mesh axis runs over, the one named last changes fastest.
Arguments:
- noise_blocks: bfloat16 [64, 12800], P('dp'), may hold values from -6 to 6
- data_blocks: bfloat16 [64, 12800], P('dp'), may hold values from -6 to 6
- destination: int32 [64], replicated, may hold values from 0 to 63, as said below
- utt_blocks: int32 [8, 4], P('dp'), may hold values from 1 to 4, 8 in all within a row
- span_start: int32 [8, 4], P('dp'), may hold values from 0 to 19
- span_size: int32 [8, 4], P('dp'), may hold values from 44 to 64
- timestep: int32 [8, 4], P('dp'), may hold values from 1 to 63
- in_weight: bfloat16 [200, 1024], replicated, may hold values from -0.4375 to 0.4375
- norm_gain: bfloat16 [1024], replicated, may hold values from 0.5 to 1.5
- qkv_weight: bfloat16 [1024, 3, 512], P(None, None, 'mp'), may hold values from -4 to 4
- out_proj: bfloat16 [512, 1024], P('mp'), may hold values from -0.25 to 0.25
- final_gain: bfloat16 [1024], replicated, may hold values from 0.25 to 1.75
- vel_weight: bfloat16 [1024, 100], replicated, may hold values from -0.1875 to 0.1875
Outputs:
- grad_qkv: float32 [1024, 3, 512], P('dp', None, 'mp')
- grad_out: float32 [512, 1024], P('mp', 'dp')
The draws below stay inside these ranges and needn't reach their ends.
Inputs may be any that keep to these rules, and one draw needn't show every extreme that they name: `destination`: A permutation of the 64 bin positions; a device sends to each bin either none or exactly 1 of its blocks.
All inputs are finite; a program needn't handle non-finite values.
Results may differ from the reference program's by a relative error of at most 0.004.
Values may be sent and summed in bfloat16 or wider, within the bound.
A program may use at most 64 MiB of HBM per device.

```python
import math
import jax
import jax.numpy as jnp
import numpy as np
from jax import lax

D = 1024
MEL = 100
HEAD_DIM = 64
BLOCK = 128
BLK_DEV = 8
INNER_WIDTH = 512
TOTAL_BLK = 64
CAP = 1
UTT_BIN = 4
MAXLEN = 4
N_DP = 8
N_MP = 4


def draw_destination(key, part):
    first, second, third, fourth, fifth = jax.random.split(key, 5)
    groups = BLK_DEV // CAP
    shifts = jax.random.permutation(first, N_DP)[:groups].astype(jnp.int32)
    outer = jax.random.permutation(second, N_DP).astype(jnp.int32)
    inner = jax.random.permutation(third, N_DP).astype(jnp.int32)
    source_order = jax.vmap(lambda k: jax.random.permutation(k, BLK_DEV))(jax.random.split(fourth, N_DP)).astype(jnp.int32)
    slot_order = jax.vmap(lambda k: jax.random.permutation(k, BLK_DEV))(jax.random.split(fifth, N_DP)).astype(jnp.int32)
    group = source_order // CAP
    within = source_order % CAP
    source = jnp.arange(N_DP, dtype=jnp.int32)[:, None]
    target_bin = outer[(inner[source] + shifts[group]) % N_DP]
    slot = slot_order[target_bin, group * CAP + within]
    return (target_bin * BLK_DEV + slot).reshape(-1).astype(jnp.int32)


def draw_qkv_weight(key, part):
    first = jax.random.fold_in(jax.random.fold_in(key, 11), 0)
    base = jax.random.normal(first, (D, 3, INNER_WIDTH), jnp.float32) * D ** (-0.5)
    return jnp.clip(base, -4.0, 4.0).astype(jnp.bfloat16)


def touch_ends(result, stream_key, low, largest):
    extent = result.shape
    index_at = [jax.random.randint(jax.random.fold_in(stream_key, axis), (), 0, extent[axis]) for axis in range(len(extent))]
    result = result.at[tuple(index_at)].set(low)
    longest = extent.index(max(extent))
    index_at[longest] = (index_at[longest] + 1) % extent[longest]
    return result.at[tuple(index_at)].set(largest)


def block_scale(stream_key, dims, cuts, low, high):
    level, own = 1.0, jax.random.fold_in(stream_key, 6)
    for position, shards_of in cuts:
        draws = jnp.exp(jax.random.uniform(jax.random.fold_in(own, position), (shards_of,), jnp.float32, low / len(cuts), high / len(cuts)))
        level = level * jnp.repeat(draws, dims[position] // shards_of).reshape([-1 if axis == position else 1 for axis in range(len(dims))])
    return level


def profile(amount, total, limit, skew):
    loads = [(1 << 20) // math.isqrt(grade ** skew) + 1 for grade in range(2, amount + 1)]
    spare, counts = total - limit - (amount - 1), [1] * (amount - 1)
    while spare > 0:
        movable = [i for i in range(amount - 1) if counts[i] < limit]
        pool, budget = sum([loads[i] for i in movable]), spare
        for i in movable:
            more = min(limit - counts[i], max(1, budget * loads[i] // pool), spare)
            counts[i] = counts[i] + more
            spare = spare - more
    return np.array([limit] + counts)


def ragged_sizes(own_key, number_of, total, most, slope):
    if number_of == 2:
        one = jax.random.randint(own_key, (), max(1, total - most), min(most, total - 1) + 1)
        return jnp.stack([one, total - one])
    tallies = jnp.asarray(profile(number_of, total, most, slope), jnp.int32)
    couples = (number_of - 1) // 2
    giver, sink = tallies[1:1 + 2 * couples:2], tallies[2:2 + 2 * couples:2]
    slack = jnp.minimum(giver - 1, most - sink)
    moved = jax.random.randint(jax.random.fold_in(own_key, 1), (couples,), 0, 1 << 20) % (slack + 1)
    tallies = tallies.at[1:1 + 2 * couples:2].set(giver - moved).at[2:2 + 2 * couples:2].set(sink + moved)
    return tallies[jax.random.permutation(jax.random.fold_in(own_key, 2), number_of)]


def centred(stream_key, dims, scale, limit, pieces=(), kind=jnp.bfloat16):
    entries = jax.random.normal(stream_key, dims, jnp.float32) * scale
    if len(pieces) > 0:
        entries = block_scale(stream_key, dims, pieces, -0.22, 0.18) * entries
    return jnp.clip(entries, min=-limit, max=limit).astype(kind)


def setup_inputs(seed: int = 0) -> dict:
    arg_keys = jax.random.split(jax.random.key(seed), 14)
    noise_blocks = centred(arg_keys[0], (TOTAL_BLK, BLOCK * MEL), 1.0, 6.0, ((0, 8),))
    data_blocks = centred(arg_keys[1], (TOTAL_BLK, BLOCK * MEL), 1.0, 6.0, ((0, 8),))
    destination = draw_destination(jax.random.fold_in(arg_keys[13], 71), 0)
    utt_blocks = jax.vmap(lambda own: ragged_sizes(own, UTT_BIN, BLK_DEV, MAXLEN, 2))(jax.random.split(arg_keys[3], N_DP)).reshape((N_DP, UTT_BIN)).astype(jnp.int32)
    span_start = touch_ends(jax.random.randint(arg_keys[4], (N_DP, UTT_BIN), 0, 20), jax.random.fold_in(arg_keys[4], 1), 0, 19).astype(jnp.int32)
    span_size = touch_ends(jax.random.randint(arg_keys[5], (N_DP, UTT_BIN), 44, 65), jax.random.fold_in(arg_keys[5], 1), 44, 64).astype(jnp.int32)
    timestep = touch_ends(jax.random.randint(arg_keys[6], (N_DP, UTT_BIN), 1, 64), jax.random.fold_in(arg_keys[6], 1), 1, 63).astype(jnp.int32)
    in_weight = centred(arg_keys[7], (2 * MEL, D), (2 * MEL) ** -0.5, 0.4375)
    norm_gain = jnp.clip(1.0 + 0.1 * jax.random.normal(arg_keys[8], (D,), jnp.float32), 0.5, 1.5).astype(jnp.bfloat16)
    qkv_weight = draw_qkv_weight(jax.random.fold_in(arg_keys[13], 71), 0)
    out_proj = centred(arg_keys[10], (INNER_WIDTH, D), INNER_WIDTH ** -0.5, 0.25, ((0, 4),))
    final_gain = jnp.clip(1.0 + 0.15 * jax.random.normal(arg_keys[11], (D,), jnp.float32), 0.25, 1.75).astype(jnp.bfloat16)
    vel_weight = centred(arg_keys[12], (D, MEL), D ** -0.5, 0.1875)
    return dict(noise_blocks=noise_blocks, data_blocks=data_blocks, destination=destination, utt_blocks=utt_blocks, span_start=span_start, span_size=span_size, timestep=timestep, in_weight=in_weight, norm_gain=norm_gain, qkv_weight=qkv_weight, out_proj=out_proj, final_gain=final_gain, vel_weight=vel_weight)


def frame_table(lengths, starts, sizes, steps, rows):
    lengths = lengths.astype(jnp.int32)
    ends = jnp.cumsum(lengths).astype(jnp.int32)
    frame = jnp.arange(rows, dtype=jnp.int32)
    block_index = frame // BLOCK
    segment = lax.optimization_barrier(jnp.sum((block_index[:, None] >= ends[None, :]).astype(jnp.int32), axis=1))
    member = segment[:, None] == jnp.arange(lengths.shape[0], dtype=jnp.int32)[None, :]
    first = lax.optimization_barrier(jnp.sum(jnp.where(member, (ends - lengths)[None, :], 0), axis=1)) * BLOCK
    span = lax.optimization_barrier(jnp.sum(jnp.where(member, lengths[None, :], 0), axis=1)) * BLOCK
    lower = lax.optimization_barrier(jnp.sum(jnp.where(member, starts[None, :], 0), axis=1))
    upper = lower + lax.optimization_barrier(jnp.sum(jnp.where(member, sizes[None, :], 0), axis=1))
    inside = 64 * (frame - first)
    masked = ((inside >= lower * span) & (inside < upper * span)).astype(jnp.float32)
    level = lax.optimization_barrier(jnp.sum(jnp.where(member, steps[None, :], 0), axis=1)).astype(jnp.float32) / 64.0
    return (segment, masked, level)

def attend(query, keys, values, segment):
    rows, width = query.shape
    heads = width // HEAD_DIM
    block = min(512, rows)
    reach = min(4, rows // BLOCK // 2) * BLOCK
    window = min(rows, block + 2 * reach)
    blocks = rows // block
    query_blocks = query.reshape(blocks, block, heads, HEAD_DIM)
    segment_blocks = segment.reshape(blocks, block)
    firsts = jnp.clip(jnp.arange(blocks, dtype=jnp.int32) * block - reach, 0, rows - window).astype(jnp.int32)
    keyed = keys.reshape(rows, heads, HEAD_DIM)
    valued = values.reshape(rows, heads, HEAD_DIM)

    def one_block(item):
        query_block, segment_block, first = item
        key_block = lax.dynamic_slice_in_dim(keyed, first, window, 0)
        value_block = lax.dynamic_slice_in_dim(valued, first, window, 0)
        key_segment = lax.dynamic_slice_in_dim(segment, first, window, 0)
        scores = jnp.einsum('qhd,khd->hqk', query_block, key_block, preferred_element_type=jnp.float32) * HEAD_DIM ** (-0.5)
        scores = jnp.where((segment_block[:, None] == key_segment[None, :])[None], scores, -1e+30)
        top = lax.optimization_barrier(jnp.max(scores, axis=-1, keepdims=True))
        weights = jnp.exp(scores - top)
        probs = (weights / lax.optimization_barrier(jnp.sum(weights, axis=-1, keepdims=True))).astype(jnp.bfloat16)
        return jnp.einsum('hqk,khd->qhd', probs, value_block, preferred_element_type=jnp.float32).reshape(block, width)
    return lax.map(jax.checkpoint(one_block), (query_blocks, segment_blocks, firsts)).reshape(rows, width)

def reference(noise_blocks, data_blocks, destination, utt_blocks, span_start, span_size, timestep, in_weight, norm_gain, qkv_weight, out_proj, final_gain, vel_weight):
    total = noise_blocks.shape[0]
    bins = utt_blocks.shape[0]
    per_bin = total // bins
    rows = per_bin * BLOCK
    mel = noise_blocks.shape[1] // BLOCK
    ordered_noise = jnp.zeros_like(noise_blocks).at[destination].set(noise_blocks)
    ordered_data = jnp.zeros_like(data_blocks).at[destination].set(data_blocks)
    group_width = INNER_WIDTH // N_MP
    gain_out = final_gain.astype(jnp.float32)[None, :]

    def one_bin(carry, index):
        grad_qkv, grad_out, count = carry
        noise = lax.dynamic_slice_in_dim(ordered_noise, index * per_bin, per_bin, 0).reshape(rows, mel).astype(jnp.float32)
        data = lax.dynamic_slice_in_dim(ordered_data, index * per_bin, per_bin, 0).reshape(rows, mel).astype(jnp.float32)
        lengths = lax.dynamic_index_in_dim(utt_blocks, index, 0, keepdims=False)
        starts = lax.dynamic_index_in_dim(span_start, index, 0, keepdims=False)
        sizes = lax.dynamic_index_in_dim(span_size, index, 0, keepdims=False)
        steps = lax.dynamic_index_in_dim(timestep, index, 0, keepdims=False)
        segment, masked, level = frame_table(lengths, starts, sizes, steps, rows)
        noisy = (1.0 - level[:, None]) * noise + level[:, None] * data
        cond = data * (1.0 - masked[:, None])
        target = data - noise
        inputs = jnp.concatenate([noisy, cond], axis=1).astype(jnp.bfloat16)
        hidden0 = jnp.dot(inputs, in_weight, preferred_element_type=jnp.float32)
        scale = lax.rsqrt(lax.optimization_barrier(jnp.mean(hidden0 * hidden0, axis=1, keepdims=True)) + 1e-06)
        normed = (hidden0 * scale * norm_gain.astype(jnp.float32)[None, :]).astype(jnp.bfloat16)
        query = jnp.dot(normed, qkv_weight[:, 0, :], preferred_element_type=jnp.float32).astype(jnp.bfloat16)
        keys = jnp.dot(normed, qkv_weight[:, 1, :], preferred_element_type=jnp.float32).astype(jnp.bfloat16)
        values = jnp.dot(normed, qkv_weight[:, 2, :], preferred_element_type=jnp.float32).astype(jnp.bfloat16)
        heads_out, pullback = jax.vjp(lambda a, b, c: attend(a, b, c, segment), query, keys, values)
        attended = heads_out.astype(jnp.bfloat16)
        mixed = jnp.zeros((rows, D), jnp.float32)
        for group in range(N_MP):
            lo = group * group_width
            part = jnp.dot(attended[:, lo:lo + group_width], out_proj[lo:lo + group_width, :], preferred_element_type=jnp.float32)
            mixed = mixed + part.astype(jnp.bfloat16).astype(jnp.float32)
        hidden1 = (hidden0 + mixed).astype(jnp.bfloat16)
        wide1 = lax.optimization_barrier(hidden1).astype(jnp.float32)
        rscale = lax.rsqrt(lax.optimization_barrier(jnp.mean(wide1 * wide1, axis=1, keepdims=True)) + 1e-06)
        normalized = wide1 * rscale
        final = (normalized * gain_out).astype(jnp.bfloat16)
        velocity = jnp.dot(final, vel_weight, preferred_element_type=jnp.float32)
        error = (2.0 * masked[:, None] * (velocity - target)).astype(jnp.bfloat16)
        grad_final = jnp.dot(error, vel_weight.T, preferred_element_type=jnp.float32)
        scaled = grad_final * gain_out
        back1 = (rscale * (scaled - normalized * lax.optimization_barrier(jnp.mean(scaled * normalized, axis=1, keepdims=True)))).astype(jnp.bfloat16)
        back_att = jnp.dot(back1, out_proj.T, preferred_element_type=jnp.float32).astype(jnp.bfloat16)
        dquery, dkeys, dvalues = pullback(back_att.astype(jnp.float32))
        grad_out = grad_out + jnp.dot(attended.T, back1, preferred_element_type=jnp.float32)
        terms = jnp.stack([jnp.dot(normed.T, dquery, preferred_element_type=jnp.float32), jnp.dot(normed.T, dkeys, preferred_element_type=jnp.float32), jnp.dot(normed.T, dvalues, preferred_element_type=jnp.float32)], axis=1)
        return ((grad_qkv + terms, grad_out, count + jnp.sum(masked)), None)
    start = (jnp.zeros((D, 3, INNER_WIDTH), jnp.float32), jnp.zeros((INNER_WIDTH, D), jnp.float32), jnp.zeros((), jnp.float32))
    (grad_qkv, grad_out, count), _ = lax.scan(one_bin, start, jnp.arange(bins, dtype=jnp.int32))
    return (grad_qkv / count, grad_out / count)
```

```python
import functools

import jax
import jax.numpy as jnp
from jax import lax
from jax.experimental import pallas as pl
from jax.experimental.pallas import tpu as pltpu
from jax.sharding import PartitionSpec as P

HEAD_DIM = 64
BLOCK = 128
LANES = 128
LONGEST = 4
MESH = pl.DeviceIdType.MESH
VMEM = pl.BlockSpec(memory_space=pltpu.VMEM)
SMEM = pl.BlockSpec(memory_space=pltpu.SMEM)
ANY = pl.BlockSpec(memory_space=pl.ANY)
F32, BF16, I32 = jnp.float32, jnp.bfloat16, jnp.int32
NN = (((1,), (0,)), ((), ()))
NT = (((1,), (1,)), ((), ()))
TN = (((0,), (0,)), ((), ()))


def dot(a, b, dims=NN):
    return lax.dot_general(a, b, dims, preferred_element_type=F32)


def params(**kw):
    return pltpu.CompilerParams(vmem_limit_bytes=56 * 2**20, **kw)


def greet(dp, mp):
    me, my = lax.axis_index("dp"), lax.axis_index("mp")
    barrier = pltpu.get_barrier_semaphore()
    for i in range(1, dp):
        pl.semaphore_signal(
            barrier, inc=1, device_id=(lax.rem(me + i, dp), my), device_id_type=MESH
        )
    for i in range(1, mp):
        pl.semaphore_signal(
            barrier, inc=1, device_id=(me, lax.rem(my + i, mp)), device_id_type=MESH
        )
    return lambda: pl.semaphore_wait(barrier, dp - 1 + mp - 1)


def remote(src, dst, send, recv, device):
    return pltpu.make_async_remote_copy(
        src, dst, send, recv, device_id=device, device_id_type=MESH
    )


PIECES = 2
SLOT_AT, POS, SOURCE, FIRST, LENGTH, LOW, HIGH, STEP = range(8)


def step_kernel(
    dp, mp,
    dest_ref, utt_ref, start_ref, size_ref, step_ref,
    x_hbm, win_hbm, gain_ref, wqkv_hbm, own_hbm, gain2_ref, vel_hbm,
    out_ref, out2_ref,
    x_ref, win_ref, wpad, wqkv, wcat, own_ref, vel_ref, lsem, tall_ref,
    stage, got, tally, tab, out_full,
    hid_ref, normed_ref, qkv_ref, p_ref, pb_ref, att_ref, all_ref, back_ref,
    dosend, do_rel, do_ref, ds_ref, dt_ref,
    okeep, osend, onear, osum, ofar,
    tkeep, tsend, tnear, tsum, tfar,
    ukeep, usend, unear, usum, ufar,
    fsend, frecv, csend, crecv, hsend, hrecv,
    wsend, wrecv, wfsend, wfrecv,
    asend, arecv, dsend, drecv, o1s, o1r, o2s, o2r,
    t1s, t1r, t2s, t2r, u1s, u1r, u2s, u2r,
):
    me, my = lax.axis_index("dp"), lax.axis_index("mp")
    slots = normed_ref.shape[0]
    features = normed_ref.shape[2]
    width = own_ref.shape[0]
    mel = x_ref.shape[3]
    share = slots // mp
    pair, side = my // 2, lax.rem(my, 2)
    pairs = mp // 2
    mate = pair * 2 + 1 - side
    group, half = me // 2, lax.rem(me, 2)
    groups = dp // 2
    partner = group * 2 + 1 - half
    aligned = dp == slots

    wait = greet(dp, mp)
    loads = [
        pltpu.make_async_copy(a, b, lsem.at[n]) for n, (a, b) in enumerate((
            (x_hbm, x_ref), (win_hbm, win_ref), (wqkv_hbm, wqkv), (own_hbm, own_ref), (vel_hbm, vel_ref),
        ))
    ]
    for c in loads:
        c.start()
    owners = [dest_ref[me * slots + k] // slots for k in range(slots)]
    stage[...] = jnp.zeros_like(stage)
    loads[0].wait()
    for i in range(dp):
        to = lax.rem(me + i, dp)
        pick = jnp.int32(0)
        for k in range(slots):
            pick = jnp.where(owners[k] == to, k, pick)
        for part in range(2):
            stage[i, part, :, 0:mel] = x_ref[part, pick]
    count = jnp.int32(0)
    for u in range(utt_ref.shape[1]):
        low = start_ref[0, u]
        high = jnp.minimum(low + size_ref[0, u], 64)
        count += (high - low) * utt_ref[0, u] * (BLOCK // 64)
    tally[0] = jnp.full(tally.shape[1:], count, I32).astype(F32)
    got[0] = stage[0]
    lines = pl.ds(pl.multiple_of(side * (BLOCK // 2), BLOCK // 2), BLOCK // 2)
    wait()

    def frame_copy(i):
        return remote(
            stage.at[i, :, lines], got.at[i, :, lines], fsend.at[i], frecv.at[i],
            (lax.rem(me + i, dp), my),
        )

    def onward(i):
        return remote(
            got.at[i, :, lines], got.at[i, :, lines], hsend.at[i], hrecv.at[i], (me, mate)
        )

    def count_copy(i):
        return remote(tally.at[0], tally.at[i], csend.at[i], crecv.at[i], (lax.rem(me + i, dp), my))

    order = sorted(range(1, dp), key=lambda i: -min(i, dp - i))
    for i in order:
        frame_copy(i).start()
    for i in order:
        count_copy(i).start()
    loads[3].wait()
    piece = width // PIECES

    def full_at(a, b, p):
        return out_full.at[a, b, pl.ds(p * piece, piece)]

    def device_at(a, b):
        return (me, lax.rem(pair + pairs - a, pairs) * 2 + lax.rem(side + b, 2))

    def mine(p):
        return own_ref.at[pl.ds(p * piece, piece)]

    across = [
        remote(mine(p), full_at(c, 0, p), wsend.at[c, p], wrecv.at[c, p], device_at(pairs - c, 0))
        for p in range(PIECES) for c in range(1, pairs)
    ]
    beside = [
        remote(mine(p), full_at(0, 1, p), wsend.at[0, p], wrecv.at[0, p], (me, mate))
        for p in range(PIECES)
    ]
    for c in across + beside:
        c.start()
    out_full[0, 0] = own_ref[...]

    def find(i, found):
        d = dest_ref[i]
        return tuple(jnp.where(d == me * slots + j, i // slots, o) for j, o in enumerate(found))

    origin = lax.fori_loop(0, dp * slots, find, (jnp.int32(0),) * slots)
    origin = [lax.rem(me + dp - o, dp) for o in origin]
    for s in range(slots):
        if aligned:
            tab[SLOT_AT, s] = origin[s]
            pos = jnp.int32(0)
            for j in range(slots):
                pos = jnp.where(origin[j] == s, j, pos)
        else:
            tab[SLOT_AT, s] = jnp.int32(s)
            tab[SOURCE, s] = origin[s]
            pos = jnp.int32(s)
        at = first = length = low = high = step = jnp.int32(0)
        for u in range(utt_ref.shape[1]):
            n = utt_ref[0, u]
            inside = (pos >= at) & (pos < at + n)
            first = jnp.where(inside, at, first)
            length = jnp.where(inside, n, length)
            low = jnp.where(inside, start_ref[0, u] * n * (BLOCK // 64), low)
            high = jnp.where(inside, (start_ref[0, u] + size_ref[0, u]) * n * (BLOCK // 64), high)
            step = jnp.where(inside, step_ref[0, u], step)
            at = at + n
        tab[POS, s] = pos
        tab[FIRST, s] = first
        tab[LENGTH, s] = length
        tab[LOW, s] = low
        tab[HIGH, s] = high
        tab[STEP, s] = step

    loads[1].wait()
    wpad[...] = jnp.zeros_like(wpad)
    wpad[0:mel] = win_ref[0:mel]
    wpad[LANES : LANES + mel] = win_ref[mel : 2 * mel]
    loads[2].wait()
    for j in range(3):
        wcat[:, j * width : (j + 1) * width] = wqkv[j]
    gain = gain_ref[...].astype(F32).reshape(1, -1)

    def masked_of(s):
        frame = (tab[POS, s] - tab[FIRST, s]) * BLOCK + lax.broadcasted_iota(I32, (BLOCK, 1), 0)
        return ((frame >= tab[LOW, s]) & (frame < tab[HIGH, s])).astype(F32)

    def inputs_of(s):
        src = s if aligned else tab[SOURCE, s]
        noise, data = got[src, 0].astype(F32), got[src, 1].astype(F32)
        level = jnp.full((1, 1), tab[STEP, s], I32).astype(F32) / 64.0
        noisy = (1.0 - level) * noise + level * data
        cond = data * (1.0 - masked_of(s))
        return jnp.concatenate([noisy, cond], axis=1).astype(BF16)

    def encode(pieces):
        hidden = dot(jnp.concatenate([inputs_of(s) for s in pieces], axis=0), wpad[...])
        scale = lax.rsqrt(jnp.mean(hidden * hidden, axis=1, keepdims=True) + 1e-06)
        normed = (hidden * scale * gain).astype(BF16)
        qkv = dot(normed, wcat[...]).astype(BF16)
        for n, s in enumerate(pieces):
            rows = slice(n * BLOCK, (n + 1) * BLOCK)
            hid_ref[s] = hidden[rows]
            normed_ref[s] = normed[rows]
            qkv_ref[s] = qkv[rows]

    def receive(pieces):
        for i in pieces:
            if i:
                frame_copy(i).wait_recv()
                onward(i).start()

    def settle(pieces):
        for i in pieces:
            if i:
                onward(i).wait_recv()

    near_first = [0] + order[::-1]
    rounds = [near_first[n : n + 2] for n in range(0, dp, 2)]
    if aligned:
        receive(rounds[0])
        for n, pieces in enumerate(rounds):
            if n + 1 < len(rounds):
                receive(rounds[n + 1])
            settle(pieces)
            encode(pieces)
    else:
        for pieces in rounds:
            receive(pieces)
        for pieces in rounds:
            settle(pieces)
        for n in range(0, slots, 2):
            encode([n, n + 1])

    passed = []
    for p in range(PIECES):
        for c in range(1, pairs):
            across[p * (pairs - 1) + c - 1].wait_recv()
            f = remote(full_at(c, 0, p), full_at(c, 1, p), wfsend.at[c, p], wfrecv.at[c, p], (me, mate))
            f.start()
            passed.append(f)

    window = min(LONGEST, slots)
    heads = width // HEAD_DIM
    lane = lax.broadcasted_iota(I32, (1, width), 1) // HEAD_DIM
    masks = [lane == h for h in range(heads)]

    def split(a):
        return jnp.concatenate([jnp.where(m, a, BF16(0)) for m in masks], axis=0)

    def merge(o):
        out = o[0:BLOCK]
        for h in range(1, heads):
            out = jnp.where(masks[h], o[h * BLOCK : (h + 1) * BLOCK], out)
        return out

    def window_of(s):
        begin = jnp.minimum(tab[FIRST, s], slots - window)
        at = [tab[SLOT_AT, begin + i] for i in range(window)]
        valid = [
            (begin + i >= tab[FIRST, s]) & (begin + i < tab[FIRST, s] + tab[LENGTH, s])
            for i in range(window)
        ]
        return begin, at, valid

    def query_of(s):
        return split(qkv_ref[s, :, 0:width] * BF16(HEAD_DIM**-0.5))

    def window_cols(at, j):
        return jnp.concatenate([qkv_ref[i, :, j * width : (j + 1) * width] for i in at], axis=0)

    def attend(s):
        _, at, valid = window_of(s)
        place = lax.broadcasted_iota(I32, (1, window * BLOCK), 1) // BLOCK
        bias = jnp.zeros((1, window * BLOCK), F32)
        for i in range(window):
            bias = jnp.where(place == i, jnp.where(valid[i], F32(0), F32(-1e30)), bias)
        scores = dot(query_of(s), window_cols(at, 1), NT) + bias
        e = jnp.exp(scores - jnp.max(scores, axis=1, keepdims=True))
        probs = e * (1.0 / jnp.sum(e, axis=1, keepdims=True))
        p_ref[s] = probs
        short = probs.astype(BF16)
        for i in range(window):
            pb_ref[s, i] = short[:, i * BLOCK : (i + 1) * BLOCK]
        return merge(dot(short, window_cols(at, 2))).astype(BF16)

    spots = [(a, b) for a in range(pairs - 1, -1, -1) for b in (1, 0)]
    others = spots[:-1]

    def first_slot(a, b):
        return device_at(a, b)[1] * share

    def att_copy(a, b, i):
        return remote(
            att_ref.at[a, b, i], all_ref.at[a, b, i], asend.at[a, b, i], arecv.at[a, b, i],
            device_at(pairs - a, b),
        )

    for a, b in others:
        for i in range(share):
            att_ref[a, b, i] = attend(first_slot(pairs - a, b) + i)
            att_copy(a, b, i).start()
    for i in range(share):
        all_ref[0, 0, i] = attend(my * share + i)
    for c in beside:
        c.wait_recv()
    for f in passed:
        f.wait_recv()
    loads[4].wait()
    gain2 = gain2_ref[...].astype(F32).reshape(1, -1)
    for a, b in others:
        for i in range(share):
            att_copy(a, b, i).wait_recv()
    full = jnp.concatenate([out_full[a, b] for a, b in spots], axis=0)

    def do_copy(a, b, i):
        back_a = (pairs - a) % pairs
        return remote(
            dosend.at[a, b, i], do_rel.at[back_a, b, i], dsend.at[a, b, i], drecv.at[back_a, b, i],
            device_at(a, b),
        )

    for i in range(share):
        s = my * share + i
        mixed = None
        for a, b in spots:
            part = dot(all_ref[a, b, i], out_full[a, b]).astype(BF16).astype(F32)
            mixed = part if mixed is None else mixed + part
        wide = (hid_ref[s] + mixed).astype(BF16).astype(F32)
        rscale = lax.rsqrt(jnp.mean(wide * wide, axis=1, keepdims=True) + 1e-06)
        normalized = wide * rscale
        velocity = dot((normalized * gain2).astype(BF16), vel_ref[...], NT)
        src = s if aligned else tab[SOURCE, s]
        target = (got[src, 1].astype(F32) - got[src, 0].astype(F32))[:, 0:mel]
        error = (2.0 * masked_of(s) * (velocity - target)).astype(BF16)
        scaled = dot(error, vel_ref[...]) * gain2
        back = (
            rscale * (scaled - normalized * jnp.mean(scaled * normalized, axis=1, keepdims=True))
        ).astype(BF16)
        back_ref[i] = back
        do = dot(back, full, NT).astype(BF16)
        for n, (a, b) in enumerate(spots):
            piece_do = do[:, n * width : (n + 1) * width]
            if (a, b) == (0, 0):
                do_ref[s] = piece_do
            else:
                dosend[a, b, i] = piece_do
                do_copy(a, b, i).start()

    back = jnp.concatenate([back_ref[i] for i in range(share)], axis=0)

    def out_term(a, b):
        return dot(jnp.concatenate([all_ref[a, b, i] for i in range(share)], axis=0), back, TN)

    def o_first(c):
        return remote(osend.at[c], onear.at[c], o1s.at[c], o1r.at[c], (me, mate))

    def o_second(c):
        return remote(osum.at[c], ofar.at[c], o2s.at[c], o2r.at[c], device_at(c, 0))

    for c in range(pairs - 1, -1, -1):
        osend[c] = out_term(c, 1).astype(BF16)
        o_first(c).start()
    for c in range(pairs):
        okeep[c] = out_term(c, 0)

    for u, (a, b) in enumerate(spots[::-1]):
        if u == 2:
            for c in range(1, pairs):
                o_first(c).wait_recv()
                osum[c] = (okeep[c] + onear[c].astype(F32)).astype(BF16)
                o_second(c).start()
        for i in range(share):
            s = first_slot(a, b) + i
            if u:
                do_copy((pairs - a) % pairs, b, i).wait_recv()
                do_ref[s] = do_rel[a, b, i]
        for i in range(share):
            s = first_slot(a, b) + i
            _, at, _ = window_of(s)
            probs = p_ref[s]
            dprobs = dot(split(do_ref[s]), window_cols(at, 2), NT).astype(BF16).astype(F32)
            ds = (probs * (dprobs - jnp.sum(dprobs * probs, axis=1, keepdims=True))).astype(BF16)
            for n in range(window):
                ds_ref[s, n] = ds[:, n * BLOCK : (n + 1) * BLOCK]
            dq = merge(dot(ds, window_cols(at, 1))) * (HEAD_DIM**-0.5)
            dt_ref[s, 0:width] = dq.T.astype(BF16)

    def keys_step(s, _):
        begin, at, valid = window_of(s)
        own = jnp.clip(tab[POS, s] - begin, 0, window - 1)

        def pick(ref):
            return jnp.concatenate(
                [jnp.where(valid[i], ref[at[i], own], BF16(0)) for i in range(window)], axis=0
            )

        queries = jnp.concatenate([query_of(i) for i in at], axis=0)
        couts = jnp.concatenate([split(do_ref[i]) for i in at], axis=0)
        dt_ref[s, width : 2 * width] = dot(queries, pick(ds_ref), TN).astype(BF16)
        dt_ref[s, 2 * width :] = dot(couts, pick(pb_ref), TN).astype(BF16)
        return 0

    lax.fori_loop(0, slots, keys_step, 0)

    d_all = jnp.concatenate([dt_ref[s] for s in range(slots)], axis=1)

    def t_first(i):
        return remote(tsend.at[i], tnear.at[i], t1s.at[i], t1r.at[i], (partner, my))

    def t_second(i):
        g = lax.rem(group + i, groups)
        return remote(tsum.at[i], tfar.at[i], t2s.at[i], t2r.at[i], (g * 2 + half, my))

    def u_first(i):
        return remote(usend.at[i], unear.at[i], u1s.at[i], u1r.at[i], (partner, my))

    def u_second(i):
        g = lax.rem(group + i, groups)
        return remote(usum.at[i], ufar.at[i], u2s.at[i], u2r.at[i], (g * 2 + half, my))

    cols = features // dp
    flat = cols % LANES == 0

    def columns(owner):
        return pl.ds(pl.multiple_of(owner * cols, cols), cols)

    if flat:
        def term(owner):
            normed = jnp.concatenate([normed_ref[s, :, columns(owner)] for s in range(slots)], axis=0)
            return dot(d_all, normed)
    else:
        normed_all = jnp.concatenate([normed_ref[s] for s in range(slots)], axis=0)
        for j in range(3):
            rows = d_all[j * width : (j + 1) * width]
            tall_ref[:, j * width : (j + 1) * width] = dot(rows, normed_all).T

        def term(owner):
            return tall_ref[columns(owner), 0 : 3 * width]

    far_first = sorted(range(1, groups), key=lambda i: -min(i, groups - i)) + [0]
    for i in far_first:
        g = lax.rem(group + i, groups)
        tsend[i] = term(g * 2 + 1 - half).astype(BF16)
        t_first(i).start()
        tkeep[i] = term(g * 2 + half)
    o_first(0).wait_recv()
    total = okeep[0] + onear[0].astype(F32)
    for c in range(1, pairs):
        o_second(c).wait_recv()
        total += ofar[c].astype(F32)
    if flat:
        okeep[0] = total
    else:
        tall_ref[:, 3 * width :] = total.T

    def out_piece(owner):
        return okeep[0, :, columns(owner)] if flat else tall_ref[columns(owner), 3 * width :]

    for i in far_first:
        g = lax.rem(group + i, groups)
        usend[i] = out_piece(g * 2 + 1 - half).astype(BF16)
        u_first(i).start()
        ukeep[i] = out_piece(g * 2 + half)
    for i in far_first[:-1]:
        t_first(i).wait_recv()
        tsum[i] = (tkeep[i] + tnear[i].astype(F32)).astype(BF16)
        t_second(i).start()
    for i in far_first[:-1]:
        u_first(i).wait_recv()
        usum[i] = (ukeep[i] + unear[i].astype(F32)).astype(BF16)
        u_second(i).start()
    for i in range(1, dp):
        count_copy(i).wait_recv()
    inverse = 1.0 / jnp.sum(tally[...], axis=0)[0:1]
    t_first(0).wait_recv()
    total = tkeep[0] + tnear[0].astype(F32)
    for i in far_first[:-1]:
        t_second(i).wait_recv()
        total += tfar[i].astype(F32)
    for j in range(3):
        part = total[j * width : (j + 1) * width].T if flat else total[:, j * width : (j + 1) * width]
        out_ref[j] = part * inverse
    u_first(0).wait_recv()
    total = ukeep[0] + unear[0].astype(F32)
    for i in far_first[:-1]:
        u_second(i).wait_recv()
        total += ufar[i].astype(F32)
    out2_ref[...] = (total if flat else total.T) * inverse[:, 0:1]

    for i in range(1, dp):
        frame_copy(i).wait_send()
        count_copy(i).wait_send()
        onward(i).wait_send()
    for c in across + beside + passed:
        c.wait_send()
    for a, b in others:
        for i in range(share):
            att_copy(a, b, i).wait_send()
            do_copy(a, b, i).wait_send()
    for c in range(pairs):
        o_first(c).wait_send()
        if c:
            o_second(c).wait_send()
    for i in range(groups):
        t_first(i).wait_send()
        u_first(i).wait_send()
        if i:
            t_second(i).wait_send()
            u_second(i).wait_send()


def finish_kernel(a_ref, b_ref, qkv_ref, o_ref):
    qkv_ref[...] = a_ref[...]
    o_ref[...] = b_ref[...]


def shards(
    dp, mp, noise_blocks, data_blocks, destination, utt_blocks, span_start, span_size, timestep,
    in_weight, norm_gain, qkv_weight, out_proj, final_gain, vel_weight,
):
    slots = noise_blocks.shape[0]
    mel = noise_blocks.shape[1] // BLOCK
    features = in_weight.shape[1]
    width = qkv_weight.shape[2]
    window = min(LONGEST, slots)
    heads = width // HEAD_DIM
    share, cols = slots // mp, features // dp
    pairs, groups = mp // 2, dp // 2
    flat = cols % LANES == 0
    big = (3 * width, cols) if flat else (cols, 3 * width)
    small = (width, cols) if flat else (cols, width)
    frames = jnp.concatenate([noise_blocks, data_blocks], axis=0).reshape(2, slots, BLOCK, mel)

    def array(shape, kind):
        return jax.ShapeDtypeStruct(shape, kind)

    def f32(*shape):
        return pltpu.VMEM(shape, F32)

    def bf16(*shape):
        return pltpu.VMEM(shape, BF16)

    def dma(*shape):
        return pltpu.SemaphoreType.DMA(shape)

    scratch = [
        bf16(2, slots, BLOCK, mel), bf16(2 * mel, features), bf16(2 * LANES, features),
        bf16(3, features, width), bf16(features, 3 * width), bf16(width, features), bf16(mel, features),
        dma(5), f32(8 if flat else features, 4 * width),
        bf16(dp, 2, BLOCK, LANES), bf16(dp, 2, BLOCK, LANES), f32(dp, 8, LANES),
        pltpu.SMEM((8, slots), I32), bf16(pairs, 2, width, features),
        f32(slots, BLOCK, features), bf16(slots, BLOCK, features), bf16(slots, BLOCK, 3 * width),
        f32(slots, heads * BLOCK, window * BLOCK), bf16(slots, window, heads * BLOCK, BLOCK),
        bf16(pairs, 2, share, BLOCK, width), bf16(pairs, 2, share, BLOCK, width),
        bf16(share, BLOCK, features), bf16(pairs, 2, share, BLOCK, width),
        bf16(pairs, 2, share, BLOCK, width), bf16(slots, BLOCK, width),
        bf16(slots, window, heads * BLOCK, BLOCK), bf16(slots, 3 * width, BLOCK),
        f32(pairs, width, features), bf16(pairs, width, features), bf16(pairs, width, features),
        bf16(pairs, width, features), bf16(pairs, width, features),
        f32(groups, *big), *[bf16(groups, *big)] * 4, f32(groups, *small), *[bf16(groups, *small)] * 4,
    ]
    scratch += [dma(dp)] * 6 + [dma(pairs, PIECES)] * 4 + [dma(pairs, 2, share)] * 4 + [dma(pairs)] * 4
    scratch += [dma(groups)] * 8
    sums, out_sum = pl.pallas_call(
        functools.partial(step_kernel, dp, mp),
        out_shape=(array((3, cols, width), F32), array((width, cols), F32)),
        in_specs=[SMEM] * 5 + [ANY, ANY, VMEM, ANY, ANY, VMEM, ANY],
        out_specs=(VMEM, VMEM),
        scratch_shapes=scratch,
        compiler_params=params(collective_id=0, has_side_effects=True),
        name="train_step",
    )(
        destination, utt_blocks, span_start, span_size, timestep, frames, in_weight, norm_gain,
        qkv_weight.transpose(1, 0, 2), out_proj, final_gain, vel_weight.T,
    )
    grad_qkv, grad_out = pl.pallas_call(
        finish_kernel,
        out_shape=(array((3, cols, width), F32), array((width, cols), F32)),
        in_specs=[VMEM, VMEM],
        out_specs=(VMEM, VMEM),
        compiler_params=params(),
        name="finish",
    )(sums, out_sum)
    return grad_qkv.transpose(1, 0, 2), grad_out


def solution(mesh):
    in_specs = (
        P("dp", None), P("dp", None), P(), P("dp", None), P("dp", None), P("dp", None),
        P("dp", None), P(), P(), P(None, None, "mp"), P("mp", None), P(), P(),
    )
    out_specs = (P("dp", None, "mp"), P("mp", "dp"))
    return jax.shard_map(
        functools.partial(shards, mesh.shape["dp"], mesh.shape["mp"]),
        mesh=mesh, in_specs=in_specs, out_specs=out_specs, check_vma=False,
    )
```

```python
import functools
import math

import jax
import jax.numpy as jnp
from jax import lax
from jax.experimental import pallas as pl
from jax.experimental.pallas import tpu as pltpu
from jax.sharding import PartitionSpec as P

HEAD_DIM = 64
BLOCK = 128
LANES = 128
LONGEST = 4
MESH = pl.DeviceIdType.MESH
VMEM = pl.BlockSpec(memory_space=pltpu.VMEM)
SMEM = pl.BlockSpec(memory_space=pltpu.SMEM)
ANY = pl.BlockSpec(memory_space=pl.ANY)
F32, BF16, I32 = jnp.float32, jnp.bfloat16, jnp.int32
NN = (((1,), (0,)), ((), ()))
NT = (((1,), (1,)), ((), ()))
TN = (((0,), (0,)), ((), ()))


def dot(a, b, dims=NN):
    return lax.dot_general(a, b, dims, preferred_element_type=F32)


def params(**kw):
    return pltpu.CompilerParams(vmem_limit_bytes=56 * 2**20, **kw)


def greet(dp, mp):
    me, my = lax.axis_index("dp"), lax.axis_index("mp")
    barrier = pltpu.get_barrier_semaphore()
    for i in range(1, dp):
        pl.semaphore_signal(
            barrier, inc=1, device_id=(lax.rem(me + i, dp), my), device_id_type=MESH
        )
    for i in range(1, mp):
        pl.semaphore_signal(
            barrier, inc=1, device_id=(me, lax.rem(my + i, mp)), device_id_type=MESH
        )
    return lambda: pl.semaphore_wait(barrier, dp - 1 + mp - 1)


def remote(src, dst, send, recv, device):
    return pltpu.make_async_remote_copy(
        src, dst, send, recv, device_id=device, device_id_type=MESH
    )


PIECES = 2
SLOT_AT, POS, SOURCE, FIRST, LENGTH, LOW, HIGH, STEP = range(8)


def step_kernel(
    dp, mp,
    dest_ref, utt_ref, start_ref, size_ref, step_ref,
    noise_hbm, data_hbm, win_hbm, gain_ref, wqkv_hbm, own_hbm, gain2_ref, vel_hbm,
    out_ref, out2_ref,
    noise_ref, data_ref, flat_ref, spread, framed, target_ref, win_ref, wpad, wqkv, wcat, own_ref, vel_ref, lsem, tall_ref,
    stage, got, tally, tab, out_full,
    hid_ref, normed_ref, qkv_ref, p_ref, pb_ref, att_ref, all_ref, back_ref,
    dosend, do_rel, do_ref, ds_ref, dt_ref, dv_ref,
    okeep, osend, onear, osum, ofar,
    *refs,
):
    t_refs, v_refs, u_refs = (refs[n * 5 : n * 5 + 5] + refs[33 + n * 4 : 37 + n * 4] for n in range(3))
    fsend, frecv, csend, crecv, hsend, hrecv = refs[15:21]
    wsend, wrecv, wfsend, wfrecv, asend, arecv, dsend, drecv, o1s, o1r, o2s, o2r = refs[21:33]
    me, my = lax.axis_index("dp"), lax.axis_index("mp")
    slots = normed_ref.shape[0]
    features = normed_ref.shape[2]
    width = own_ref.shape[0]
    mel = vel_ref.shape[0]
    packed = BLOCK * mel // LANES
    part_rows = got.shape[2]
    share = slots // mp
    pair, side = my // 2, lax.rem(my, 2)
    pairs = mp // 2
    mate = pair * 2 + 1 - side
    group, half = me // 2, lax.rem(me, 2)
    groups = dp // 2
    partner = group * 2 + 1 - half
    aligned = dp == slots

    wait = greet(dp, mp)
    loads = [
        pltpu.make_async_copy(a, b, lsem.at[n]) for n, (a, b) in enumerate((
            (noise_hbm, noise_ref), (data_hbm, data_ref), (win_hbm, win_ref), (wqkv_hbm, wqkv),
            (own_hbm, own_ref), (vel_hbm, vel_ref),
        ))
    ]
    for c in loads:
        c.start()
    owners = [dest_ref[me * slots + k] // slots for k in range(slots)]
    flat_ref[pl.ds(2 * packed * slots, (2 * part_rows - 2 * packed) * slots)] = jnp.zeros(
        ((2 * part_rows - 2 * packed) * slots, LANES), F32
    )
    loads[0].wait()
    loads[1].wait()
    for part, ref in enumerate((noise_ref, data_ref)):
        for r in range(packed):
            flat_ref[pl.ds((part * packed + r) * slots, slots)] = (
                ref[:, r * LANES : (r + 1) * LANES].astype(F32)
            )
    for i in range(dp):
        to = lax.rem(me + i, dp)
        pick = jnp.int32(0)
        for k in range(slots):
            pick = jnp.where(owners[k] == to, k, pick)
        for part in range(2):
            stage[i, part] = flat_ref[
                pl.ds(pick + part * part_rows * slots, part_rows, stride=slots)
            ].astype(BF16)
    count = jnp.int32(0)
    for u in range(utt_ref.shape[1]):
        low = start_ref[0, u]
        high = jnp.minimum(low + size_ref[0, u], 64)
        count += (high - low) * utt_ref[0, u] * (BLOCK // 64)
    tally[0] = jnp.full(tally.shape[1:], count, I32).astype(F32)
    got[0] = stage[0]
    wait()

    def frame_copy(i):
        return remote(
            stage.at[i, side], got.at[i, side], fsend.at[i], frecv.at[i],
            (lax.rem(me + i, dp), my),
        )

    def onward(i):
        return remote(
            got.at[i, side], got.at[i, side], hsend.at[i], hrecv.at[i], (me, mate)
        )

    def count_copy(i):
        return remote(tally.at[0], tally.at[i], csend.at[i], crecv.at[i], (lax.rem(me + i, dp), my))

    order = sorted(range(1, dp), key=lambda i: -min(i, dp - i))
    for i in order:
        frame_copy(i).start()
    for i in order:
        count_copy(i).start()
    loads[4].wait()
    piece = width // PIECES

    def full_at(a, b, p):
        return out_full.at[a, b, pl.ds(p * piece, piece)]

    def device_at(a, b):
        return (me, lax.rem(pair + pairs - a, pairs) * 2 + lax.rem(side + b, 2))

    def mine(p):
        return own_ref.at[pl.ds(p * piece, piece)]

    across = [
        remote(mine(p), full_at(c, 0, p), wsend.at[c, p], wrecv.at[c, p], device_at(pairs - c, 0))
        for p in range(PIECES) for c in range(1, pairs)
    ]
    beside = [
        remote(mine(p), full_at(0, 1, p), wsend.at[0, p], wrecv.at[0, p], (me, mate))
        for p in range(PIECES)
    ]
    for c in across + beside:
        c.start()
    out_full[0, 0] = own_ref[...]

    def find(i, found):
        d = dest_ref[i]
        return tuple(jnp.where(d == me * slots + j, i // slots, o) for j, o in enumerate(found))

    origin = lax.fori_loop(0, dp * slots, find, (jnp.int32(0),) * slots)
    origin = [lax.rem(me + dp - o, dp) for o in origin]
    for s in range(slots):
        if aligned:
            tab[SLOT_AT, s] = origin[s]
            pos = jnp.int32(0)
            for j in range(slots):
                pos = jnp.where(origin[j] == s, j, pos)
        else:
            tab[SLOT_AT, s] = jnp.int32(s)
            tab[SOURCE, s] = origin[s]
            pos = jnp.int32(s)
        at = first = length = low = high = step = jnp.int32(0)
        for u in range(utt_ref.shape[1]):
            n = utt_ref[0, u]
            inside = (pos >= at) & (pos < at + n)
            first = jnp.where(inside, at, first)
            length = jnp.where(inside, n, length)
            low = jnp.where(inside, start_ref[0, u] * n * (BLOCK // 64), low)
            high = jnp.where(inside, (start_ref[0, u] + size_ref[0, u]) * n * (BLOCK // 64), high)
            step = jnp.where(inside, step_ref[0, u], step)
            at = at + n
        tab[POS, s] = pos
        tab[FIRST, s] = first
        tab[LENGTH, s] = length
        tab[LOW, s] = low
        tab[HIGH, s] = high
        tab[STEP, s] = step

    loads[2].wait()
    wpad[...] = jnp.zeros_like(wpad)
    wpad[0:mel] = win_ref[0:mel]
    wpad[LANES : LANES + mel] = win_ref[mel : 2 * mel]
    loads[3].wait()
    for j in range(3):
        wcat[:, j * width : (j + 1) * width] = wqkv[j]
    gain = gain_ref[...].astype(F32).reshape(1, -1)

    def masked_of(s):
        frame = (tab[POS, s] - tab[FIRST, s]) * BLOCK + lax.broadcasted_iota(I32, (BLOCK, 1), 0)
        return ((frame >= tab[LOW, s]) & (frame < tab[HIGH, s])).astype(F32)

    cycle = math.lcm(mel, LANES) // mel
    turns, pitch = BLOCK // cycle, cycle + 8
    stride = cycle * mel // LANES
    lanes = lax.broadcasted_iota(I32, (1, LANES), 1)

    def frames_of(s, n):
        src = s if aligned else tab[SOURCE, s]
        for part in range(2):
            spread[n, part * part_rows : (part + 1) * part_rows] = got[src, part].astype(F32)
        for f in range(cycle):
            row, shift = f * mel // LANES, f * mel % LANES
            a = spread[n, pl.ds(row, 2 * turns, stride=stride)]
            if shift + mel > LANES:
                b = spread[n, pl.ds(row + 1, 2 * turns, stride=stride)]
                a = jnp.where(lanes >= shift, a, b)
            if shift:
                a = pltpu.roll(a, LANES - shift, axis=1)
            framed[n, pl.ds(f, 2 * turns, stride=pitch)] = a
        return [
            jnp.concatenate(
                [framed[n, (part * turns + t) * pitch : (part * turns + t) * pitch + cycle] for t in range(turns)],
                axis=0,
            )
            for part in range(2)
        ]

    def inputs_of(s, n):
        noise, data = frames_of(s, n)
        target_ref[s] = data - noise
        level = jnp.full((1, 1), tab[STEP, s], I32).astype(F32) / 64.0
        noisy = (1.0 - level) * noise + level * data
        cond = data * (1.0 - masked_of(s))
        return jnp.concatenate([noisy, cond], axis=1).astype(BF16)

    def encode(pieces):
        hidden = dot(jnp.concatenate([inputs_of(s, n) for n, s in enumerate(pieces)], axis=0), wpad[...])
        scale = lax.rsqrt(jnp.mean(hidden * hidden, axis=1, keepdims=True) + 1e-06)
        normed = (hidden * scale * gain).astype(BF16)
        qkv = dot(normed, wcat[...]).astype(BF16)
        for n, s in enumerate(pieces):
            rows = slice(n * BLOCK, (n + 1) * BLOCK)
            hid_ref[s] = hidden[rows]
            normed_ref[s] = normed[rows]
            qkv_ref[s] = qkv[rows]

    def receive(pieces):
        for i in pieces:
            if i:
                frame_copy(i).wait_recv()
                onward(i).start()

    def settle(pieces):
        for i in pieces:
            if i:
                onward(i).wait_recv()

    near_first = [0] + order[::-1]
    rounds = [near_first[n : n + 2] for n in range(0, dp, 2)]
    if aligned:
        receive(rounds[0])
        for n, pieces in enumerate(rounds):
            if n + 1 < len(rounds):
                receive(rounds[n + 1])
            settle(pieces)
            encode(pieces)
    else:
        for pieces in rounds:
            receive(pieces)
        for pieces in rounds:
            settle(pieces)
        for n in range(0, slots, 2):
            encode([n, n + 1])

    passed = []
    for p in range(PIECES):
        for c in range(1, pairs):
            across[p * (pairs - 1) + c - 1].wait_recv()
            f = remote(full_at(c, 0, p), full_at(c, 1, p), wfsend.at[c, p], wfrecv.at[c, p], (me, mate))
            f.start()
            passed.append(f)

    window = min(LONGEST, slots)
    heads = width // HEAD_DIM
    lane = lax.broadcasted_iota(I32, (1, width), 1) // HEAD_DIM
    masks = [lane == h for h in range(heads)]

    def split(a):
        return jnp.concatenate([jnp.where(m, a, BF16(0)) for m in masks], axis=0)

    def merge(o):
        out = o[0:BLOCK]
        for h in range(1, heads):
            out = jnp.where(masks[h], o[h * BLOCK : (h + 1) * BLOCK], out)
        return out

    def window_of(s):
        begin = jnp.minimum(tab[FIRST, s], slots - window)
        at = [tab[SLOT_AT, begin + i] for i in range(window)]
        valid = [
            (begin + i >= tab[FIRST, s]) & (begin + i < tab[FIRST, s] + tab[LENGTH, s])
            for i in range(window)
        ]
        return begin, at, valid

    def query_of(s):
        return split(qkv_ref[s, :, 0:width] * BF16(HEAD_DIM**-0.5))

    def window_cols(at, j):
        return jnp.concatenate([qkv_ref[i, :, j * width : (j + 1) * width] for i in at], axis=0)

    def attend(s):
        _, at, valid = window_of(s)
        place = lax.broadcasted_iota(I32, (1, window * BLOCK), 1) // BLOCK
        bias = jnp.zeros((1, window * BLOCK), F32)
        for i in range(window):
            bias = jnp.where(place == i, jnp.where(valid[i], F32(0), F32(-1e30)), bias)
        scores = dot(query_of(s), window_cols(at, 1), NT) + bias
        e = jnp.exp(scores - jnp.max(scores, axis=1, keepdims=True))
        probs = e * (1.0 / jnp.sum(e, axis=1, keepdims=True))
        p_ref[s] = probs
        short = probs.astype(BF16)
        for i in range(window):
            pb_ref[s, i] = short[:, i * BLOCK : (i + 1) * BLOCK]
        return merge(dot(short, window_cols(at, 2))).astype(BF16)

    spots = [(a, b) for a in range(pairs - 1, -1, -1) for b in (1, 0)]
    others = spots[:-1]

    def first_slot(a, b):
        return device_at(a, b)[1] * share

    def att_copy(a, b, i):
        return remote(
            att_ref.at[a, b, i], all_ref.at[a, b, i], asend.at[a, b, i], arecv.at[a, b, i],
            device_at(pairs - a, b),
        )

    for a, b in others:
        for i in range(share):
            att_ref[a, b, i] = attend(first_slot(pairs - a, b) + i)
            att_copy(a, b, i).start()
    for i in range(share):
        all_ref[0, 0, i] = attend(my * share + i)
    for c in beside:
        c.wait_recv()
    for f in passed:
        f.wait_recv()
    loads[5].wait()
    gain2 = gain2_ref[...].astype(F32).reshape(1, -1)
    for a, b in others:
        for i in range(share):
            att_copy(a, b, i).wait_recv()
    full = jnp.concatenate([out_full[a, b] for a, b in spots], axis=0)

    def do_copy(a, b, i):
        back_a = (pairs - a) % pairs
        return remote(
            dosend.at[a, b, i], do_rel.at[back_a, b, i], dsend.at[a, b, i], drecv.at[back_a, b, i],
            device_at(a, b),
        )

    for i in range(share):
        s = my * share + i
        mixed = None
        for a, b in spots:
            part = dot(all_ref[a, b, i], out_full[a, b]).astype(BF16).astype(F32)
            mixed = part if mixed is None else mixed + part
        wide = (hid_ref[s] + mixed).astype(BF16).astype(F32)
        rscale = lax.rsqrt(jnp.mean(wide * wide, axis=1, keepdims=True) + 1e-06)
        normalized = wide * rscale
        velocity = dot((normalized * gain2).astype(BF16), vel_ref[...], NT)
        error = (2.0 * masked_of(s) * (velocity - target_ref[s, :, 0:mel])).astype(BF16)
        scaled = dot(error, vel_ref[...]) * gain2
        back = (
            rscale * (scaled - normalized * jnp.mean(scaled * normalized, axis=1, keepdims=True))
        ).astype(BF16)
        back_ref[i] = back
        do = dot(back, full, NT).astype(BF16)
        for n, (a, b) in enumerate(spots):
            piece_do = do[:, n * width : (n + 1) * width]
            if (a, b) == (0, 0):
                do_ref[s] = piece_do
            else:
                dosend[a, b, i] = piece_do
                do_copy(a, b, i).start()

    back = jnp.concatenate([back_ref[i] for i in range(share)], axis=0)

    def out_term(a, b):
        return dot(jnp.concatenate([all_ref[a, b, i] for i in range(share)], axis=0), back, TN)

    def o_first(c):
        return remote(osend.at[c], onear.at[c], o1s.at[c], o1r.at[c], (me, mate))

    def o_second(c):
        return remote(osum.at[c], ofar.at[c], o2s.at[c], o2r.at[c], device_at(c, 0))

    for c in range(pairs - 1, -1, -1):
        osend[c] = out_term(c, 1).astype(BF16)
        o_first(c).start()
    for c in range(pairs):
        okeep[c] = out_term(c, 0)

    for u, (a, b) in enumerate(spots[::-1]):
        for i in range(share):
            if u:
                do_copy((pairs - a) % pairs, b, i).wait_recv()
                do_ref[first_slot(a, b) + i] = do_rel[a, b, i]

    def pick(ref, s):
        begin, at, valid = window_of(s)
        own = jnp.clip(tab[POS, s] - begin, 0, window - 1)
        return at, jnp.concatenate(
            [jnp.where(valid[i], ref[at[i], own], BF16(0)) for i in range(window)], axis=0
        )

    def values_step(s, _):
        at, probs = pick(pb_ref, s)
        couts = jnp.concatenate([split(do_ref[i]) for i in at], axis=0)
        dv_ref[s] = dot(couts, probs, TN).astype(BF16)
        return 0

    lax.fori_loop(0, slots, values_step, 0, unroll=2)

    for c in range(1, pairs):
        o_first(c).wait_recv()
        osum[c] = (okeep[c] + onear[c].astype(F32)).astype(BF16)
        o_second(c).start()

    cols = features // dp
    flat = cols % LANES == 0
    far_first = sorted(range(1, groups), key=lambda i: -min(i, groups - i)) + [0]

    def columns(owner):
        return pl.ds(pl.multiple_of(owner * cols, cols), cols)

    class Reduction:
        def __init__(self, refs, term):
            self.keep, self.out, self.near, self.sum, self.far, *self.sems = refs
            self.term = term

        def first(self, i):
            s1, r1, _, _ = self.sems
            return remote(self.out.at[i], self.near.at[i], s1.at[i], r1.at[i], (partner, my))

        def second(self, i):
            _, _, s2, r2 = self.sems
            g = lax.rem(group + i, groups)
            return remote(self.sum.at[i], self.far.at[i], s2.at[i], r2.at[i], (g * 2 + half, my))

        def begin(self):
            for i in far_first:
                g = lax.rem(group + i, groups)
                self.out[i] = self.term(g * 2 + 1 - half).astype(BF16)
                self.first(i).start()
                self.keep[i] = self.term(g * 2 + half)

        def middle(self):
            for i in far_first[:-1]:
                self.first(i).wait_recv()
                self.sum[i] = (self.keep[i] + self.near[i].astype(F32)).astype(BF16)
                self.second(i).start()

        def end(self):
            self.first(0).wait_recv()
            total = self.keep[0] + self.near[0].astype(F32)
            for i in far_first[:-1]:
                self.second(i).wait_recv()
                total += self.far[i].astype(F32)
            return total

        def drain(self):
            for i in range(groups):
                self.first(i).wait_send()
                if i:
                    self.second(i).wait_send()

    def product(ref, at):
        parts = jnp.concatenate([ref[s] for s in range(slots)], axis=1)
        rows = parts.shape[0]
        if flat:
            return lambda owner: dot(
                parts,
                jnp.concatenate([normed_ref[s, :, columns(owner)] for s in range(slots)], axis=0),
            )
        normed = jnp.concatenate([normed_ref[s] for s in range(slots)], axis=0)
        for n in range(0, rows, width):
            tall_ref[:, at + n : at + n + width] = dot(parts[n : n + width], normed).T
        return lambda owner: tall_ref[columns(owner), at : at + rows]

    values = Reduction(v_refs, product(dv_ref, 2 * width))
    values.begin()

    for u, (a, b) in enumerate(spots[::-1]):
        if u == mp // 2:
            values.middle()
        for i in range(share):
            s = first_slot(a, b) + i
            _, at, _ = window_of(s)
            probs = p_ref[s]
            dprobs = dot(split(do_ref[s]), window_cols(at, 2), NT).astype(BF16).astype(F32)
            ds = (probs * (dprobs - jnp.sum(dprobs * probs, axis=1, keepdims=True))).astype(BF16)
            for n in range(window):
                ds_ref[s, n] = ds[:, n * BLOCK : (n + 1) * BLOCK]
            dq = merge(dot(ds, window_cols(at, 1))) * (HEAD_DIM**-0.5)
            dt_ref[s, 0:width] = dq.T.astype(BF16)

    def keys_step(s, _):
        at, ds = pick(ds_ref, s)
        queries = jnp.concatenate([query_of(i) for i in at], axis=0)
        dt_ref[s, width : 2 * width] = dot(queries, ds, TN).astype(BF16)
        return 0

    lax.fori_loop(0, slots, keys_step, 0, unroll=2)

    others_of = Reduction(t_refs, product(dt_ref, 0))
    others_of.begin()
    o_first(0).wait_recv()
    total = okeep[0] + onear[0].astype(F32)
    for c in range(1, pairs):
        o_second(c).wait_recv()
        total += ofar[c].astype(F32)
    if flat:
        okeep[0] = total
        outs = Reduction(u_refs, lambda owner: okeep[0, :, columns(owner)])
    else:
        tall_ref[:, 3 * width :] = total.T
        outs = Reduction(u_refs, lambda owner: tall_ref[columns(owner), 3 * width :])
    outs.begin()
    others_of.middle()
    outs.middle()
    for i in range(1, dp):
        count_copy(i).wait_recv()
    inverse = 1.0 / jnp.sum(tally[...], axis=0)[0:1]
    total = values.end()
    out_ref[2] = (total.T if flat else total) * inverse
    total = others_of.end()
    for j in range(2):
        part = total[j * width : (j + 1) * width].T if flat else total[:, j * width : (j + 1) * width]
        out_ref[j] = part * inverse
    total = outs.end()
    out2_ref[...] = (total if flat else total.T) * inverse[:, 0:1]

    for i in range(1, dp):
        frame_copy(i).wait_send()
        count_copy(i).wait_send()
        onward(i).wait_send()
    for c in across + beside + passed:
        c.wait_send()
    for a, b in others:
        for i in range(share):
            att_copy(a, b, i).wait_send()
            do_copy(a, b, i).wait_send()
    for c in range(pairs):
        o_first(c).wait_send()
        if c:
            o_second(c).wait_send()
    for reduction in (values, others_of, outs):
        reduction.drain()


def finish_kernel(a_ref, b_ref, qkv_ref, o_ref):
    qkv_ref[...] = a_ref[...]
    o_ref[...] = b_ref[...]


def shards(
    dp, mp, noise_blocks, data_blocks, destination, utt_blocks, span_start, span_size, timestep,
    in_weight, norm_gain, qkv_weight, out_proj, final_gain, vel_weight,
):
    slots = noise_blocks.shape[0]
    mel = noise_blocks.shape[1] // BLOCK
    features = in_weight.shape[1]
    width = qkv_weight.shape[2]
    window = min(LONGEST, slots)
    heads = width // HEAD_DIM
    share, cols = slots // mp, features // dp
    pairs, groups = mp // 2, dp // 2
    flat = cols % LANES == 0
    shapes = [(n * width, cols) if flat else (cols, n * width) for n in (2, 1, 1)]
    packed = BLOCK * mel // LANES
    part_rows = (packed + 7) // 8 * 8
    cycle = math.lcm(mel, LANES) // mel

    def array(shape, kind):
        return jax.ShapeDtypeStruct(shape, kind)

    def f32(*shape):
        return pltpu.VMEM(shape, F32)

    def bf16(*shape):
        return pltpu.VMEM(shape, BF16)

    def dma(*shape):
        return pltpu.SemaphoreType.DMA(shape)

    scratch = [
        bf16(slots, BLOCK * mel), bf16(slots, BLOCK * mel), f32(2 * part_rows * slots, LANES),
        f32(2, 2 * part_rows, LANES), f32(2, 2 * (BLOCK // cycle) * (cycle + 8), LANES),
        f32(slots, BLOCK, LANES), bf16(2 * mel, features), bf16(2 * LANES, features),
        bf16(3, features, width), bf16(features, 3 * width), bf16(width, features), bf16(mel, features),
        dma(6), f32(8 if flat else features, 4 * width),
        bf16(dp, 2, part_rows, LANES), bf16(dp, 2, part_rows, LANES), f32(dp, 8, LANES),
        pltpu.SMEM((8, slots), I32), bf16(pairs, 2, width, features),
        f32(slots, BLOCK, features), bf16(slots, BLOCK, features), bf16(slots, BLOCK, 3 * width),
        f32(slots, heads * BLOCK, window * BLOCK), bf16(slots, window, heads * BLOCK, BLOCK),
        bf16(pairs, 2, share, BLOCK, width), bf16(pairs, 2, share, BLOCK, width),
        bf16(share, BLOCK, features), bf16(pairs, 2, share, BLOCK, width),
        bf16(pairs, 2, share, BLOCK, width), bf16(slots, BLOCK, width),
        bf16(slots, window, heads * BLOCK, BLOCK), bf16(slots, 2 * width, BLOCK), bf16(slots, width, BLOCK),
        f32(pairs, width, features), bf16(pairs, width, features), bf16(pairs, width, features),
        bf16(pairs, width, features), bf16(pairs, width, features),
    ]
    for shape in shapes:
        scratch += [f32(groups, *shape)] + [bf16(groups, *shape)] * 4
    scratch += [dma(dp)] * 6 + [dma(pairs, PIECES)] * 4 + [dma(pairs, 2, share)] * 4 + [dma(pairs)] * 4
    scratch += [dma(groups)] * 12
    sums, out_sum = pl.pallas_call(
        functools.partial(step_kernel, dp, mp),
        out_shape=(f32(3, cols, width), f32(width, cols)),
        in_specs=[SMEM] * 5 + [ANY, ANY, ANY, VMEM, ANY, ANY, VMEM, ANY],
        out_specs=(VMEM, VMEM),
        scratch_shapes=scratch,
        compiler_params=params(collective_id=0, has_side_effects=True),
        name="train_step",
    )(
        destination, utt_blocks, span_start, span_size, timestep, noise_blocks, data_blocks,
        in_weight, norm_gain,
        qkv_weight.transpose(1, 0, 2), out_proj, final_gain, vel_weight.T,
    )
    grad_qkv, grad_out = pl.pallas_call(
        finish_kernel,
        out_shape=(array((3, cols, width), F32), array((width, cols), F32)),
        in_specs=[VMEM, VMEM],
        out_specs=(VMEM, VMEM),
        compiler_params=params(),
        name="finish",
    )(
        pltpu.with_memory_space_constraint(sums, pltpu.VMEM),
        pltpu.with_memory_space_constraint(out_sum, pltpu.VMEM),
    )
    return grad_qkv.transpose(1, 0, 2), grad_out


def solution(mesh):
    in_specs = (
        P("dp", None), P("dp", None), P(), P("dp", None), P("dp", None), P("dp", None),
        P("dp", None), P(), P(), P(None, None, "mp"), P("mp", None), P(), P(),
    )
    out_specs = (P("dp", None, "mp"), P("mp", "dp"))
    return jax.shard_map(
        functools.partial(shards, mesh.shape["dp"], mesh.shape["mp"]),
        mesh=mesh, in_specs=in_specs, out_specs=out_specs, check_vma=False,
    )
```

```python
import functools
import math

import jax
import jax.numpy as jnp
from jax import lax
from jax.experimental import pallas as pl
from jax.experimental.pallas import tpu as pltpu
from jax.sharding import PartitionSpec as P

HEAD_DIM = 64
BLOCK = 128
LANES = 128
LONGEST = 4
MESH = pl.DeviceIdType.MESH
VMEM = pl.BlockSpec(memory_space=pltpu.VMEM)
SMEM = pl.BlockSpec(memory_space=pltpu.SMEM)
ANY = pl.BlockSpec(memory_space=pl.ANY)
F32, BF16, I32 = jnp.float32, jnp.bfloat16, jnp.int32
NN = (((1,), (0,)), ((), ()))
NT = (((1,), (1,)), ((), ()))
TN = (((0,), (0,)), ((), ()))


def dot(a, b, dims=NN):
    return lax.dot_general(a, b, dims, preferred_element_type=F32)


def params(**kw):
    return pltpu.CompilerParams(vmem_limit_bytes=56 * 2**20, **kw)


def greet(dp, mp):
    me, my = lax.axis_index("dp"), lax.axis_index("mp")
    barrier = pltpu.get_barrier_semaphore()
    for i in range(1, dp):
        pl.semaphore_signal(
            barrier, inc=1, device_id=(lax.rem(me + i, dp), my), device_id_type=MESH
        )
    for i in range(1, mp):
        pl.semaphore_signal(
            barrier, inc=1, device_id=(me, lax.rem(my + i, mp)), device_id_type=MESH
        )
    return lambda: pl.semaphore_wait(barrier, dp - 1 + mp - 1)


def remote(src, dst, send, recv, device):
    return pltpu.make_async_remote_copy(
        src, dst, send, recv, device_id=device, device_id_type=MESH
    )


PIECES = 2
SLOT_AT, POS, SOURCE, FIRST, LENGTH, LOW, HIGH, STEP = range(8)


def step_kernel(
    dp, mp,
    dest_ref, utt_ref, start_ref, size_ref, step_ref,
    noise_hbm, data_hbm, win_hbm, gain_ref, wqkv_hbm, own_hbm, gain2_ref, vel_hbm,
    out_ref, out2_ref,
    noise_ref, data_ref, flat_ref, spread, framed, target_ref, win_ref, wpad, wqkv, wcat, own_ref, vel_ref, lsem, tall_ref,
    stage, got, tally, tab, out_full,
    hid_ref, normed_ref, qkv_ref, p_ref, pb_ref, att_ref, all_ref, back_ref,
    dosend, do_rel, do_ref, ds_ref, dt_ref, dv_ref,
    okeep, osend, onear, osum, ofar,
    *refs,
):
    t_refs, v_refs, u_refs = (refs[n * 3 : n * 3 + 3] + refs[27 + n * 2 : 29 + n * 2] for n in range(3))
    fsend, frecv, csend, crecv, hsend, hrecv = refs[9:15]
    wsend, wrecv, wfsend, wfrecv, asend, arecv, dsend, drecv, o1s, o1r, o2s, o2r = refs[15:27]
    me, my = lax.axis_index("dp"), lax.axis_index("mp")
    slots = normed_ref.shape[0]
    features = normed_ref.shape[2]
    width = own_ref.shape[0]
    mel = vel_ref.shape[0]
    packed = BLOCK * mel // LANES
    part_rows = got.shape[2]
    share = slots // mp
    pair, side = my // 2, lax.rem(my, 2)
    pairs = mp // 2
    mate = pair * 2 + 1 - side
    aligned = dp == slots

    wait = greet(dp, mp)
    loads = [
        pltpu.make_async_copy(a, b, lsem.at[n]) for n, (a, b) in enumerate((
            (noise_hbm, noise_ref), (data_hbm, data_ref), (win_hbm, win_ref), (wqkv_hbm, wqkv),
            (own_hbm, own_ref), (vel_hbm, vel_ref),
        ))
    ]
    for c in loads:
        c.start()
    owners = [dest_ref[me * slots + k] // slots for k in range(slots)]
    flat_ref[pl.ds(2 * packed * slots, (2 * part_rows - 2 * packed) * slots)] = jnp.zeros(
        ((2 * part_rows - 2 * packed) * slots, LANES), F32
    )
    loads[0].wait()
    loads[1].wait()
    for part, ref in enumerate((noise_ref, data_ref)):
        for r in range(packed):
            flat_ref[pl.ds((part * packed + r) * slots, slots)] = (
                ref[:, r * LANES : (r + 1) * LANES].astype(F32)
            )
    for i in range(dp):
        to = lax.rem(me + i, dp)
        pick = jnp.int32(0)
        for k in range(slots):
            pick = jnp.where(owners[k] == to, k, pick)
        for part in range(2):
            stage[i, part] = flat_ref[
                pl.ds(pick + part * part_rows * slots, part_rows, stride=slots)
            ].astype(BF16)
    count = jnp.int32(0)
    for u in range(utt_ref.shape[1]):
        low = start_ref[0, u]
        high = jnp.minimum(low + size_ref[0, u], 64)
        count += (high - low) * utt_ref[0, u] * (BLOCK // 64)
    tally[0] = jnp.full(tally.shape[1:], count, I32).astype(F32)
    got[0] = stage[0]
    wait()

    def frame_copy(i):
        return remote(
            stage.at[i, side], got.at[i, side], fsend.at[i], frecv.at[i],
            (lax.rem(me + i, dp), my),
        )

    def onward(i):
        return remote(
            got.at[i, side], got.at[i, side], hsend.at[i], hrecv.at[i], (me, mate)
        )

    def count_copy(i):
        return remote(tally.at[0], tally.at[i], csend.at[i], crecv.at[i], (lax.rem(me + i, dp), my))

    order = sorted(range(1, dp), key=lambda i: -min(i, dp - i))
    for i in order:
        frame_copy(i).start()
    for i in order:
        count_copy(i).start()
    loads[4].wait()
    piece = width // PIECES

    def full_at(a, b, p):
        return out_full.at[a, b, pl.ds(p * piece, piece)]

    def device_at(a, b):
        return (me, lax.rem(pair + pairs - a, pairs) * 2 + lax.rem(side + b, 2))

    def mine(p):
        return own_ref.at[pl.ds(p * piece, piece)]

    across = [
        remote(mine(p), full_at(c, 0, p), wsend.at[c, p], wrecv.at[c, p], device_at(pairs - c, 0))
        for p in range(PIECES) for c in range(1, pairs)
    ]
    beside = [
        remote(mine(p), full_at(0, 1, p), wsend.at[0, p], wrecv.at[0, p], (me, mate))
        for p in range(PIECES)
    ]
    for c in across + beside:
        c.start()
    out_full[0, 0] = own_ref[...]

    def find(i, found):
        d = dest_ref[i]
        return tuple(jnp.where(d == me * slots + j, i // slots, o) for j, o in enumerate(found))

    origin = lax.fori_loop(0, dp * slots, find, (jnp.int32(0),) * slots)
    origin = [lax.rem(me + dp - o, dp) for o in origin]
    for s in range(slots):
        if aligned:
            tab[SLOT_AT, s] = origin[s]
            pos = jnp.int32(0)
            for j in range(slots):
                pos = jnp.where(origin[j] == s, j, pos)
        else:
            tab[SLOT_AT, s] = jnp.int32(s)
            tab[SOURCE, s] = origin[s]
            pos = jnp.int32(s)
        at = first = length = low = high = step = jnp.int32(0)
        for u in range(utt_ref.shape[1]):
            n = utt_ref[0, u]
            inside = (pos >= at) & (pos < at + n)
            first = jnp.where(inside, at, first)
            length = jnp.where(inside, n, length)
            low = jnp.where(inside, start_ref[0, u] * n * (BLOCK // 64), low)
            high = jnp.where(inside, (start_ref[0, u] + size_ref[0, u]) * n * (BLOCK // 64), high)
            step = jnp.where(inside, step_ref[0, u], step)
            at = at + n
        tab[POS, s] = pos
        tab[FIRST, s] = first
        tab[LENGTH, s] = length
        tab[LOW, s] = low
        tab[HIGH, s] = high
        tab[STEP, s] = step

    loads[2].wait()
    wpad[...] = jnp.zeros_like(wpad)
    wpad[0:mel] = win_ref[0:mel]
    wpad[LANES : LANES + mel] = win_ref[mel : 2 * mel]
    loads[3].wait()
    for j in range(3):
        wcat[:, j * width : (j + 1) * width] = wqkv[j]
    gain = gain_ref[...].astype(F32).reshape(1, -1)

    def masked_of(s):
        frame = (tab[POS, s] - tab[FIRST, s]) * BLOCK + lax.broadcasted_iota(I32, (BLOCK, 1), 0)
        return ((frame >= tab[LOW, s]) & (frame < tab[HIGH, s])).astype(F32)

    cycle = math.lcm(mel, LANES) // mel
    turns, pitch = BLOCK // cycle, cycle + 8
    stride = cycle * mel // LANES
    lanes = lax.broadcasted_iota(I32, (1, LANES), 1)

    def frames_of(s, n):
        src = s if aligned else tab[SOURCE, s]
        for part in range(2):
            spread[n, part * part_rows : (part + 1) * part_rows] = got[src, part].astype(F32)
        for f in range(cycle):
            row, shift = f * mel // LANES, f * mel % LANES
            a = spread[n, pl.ds(row, 2 * turns, stride=stride)]
            if shift + mel > LANES:
                b = spread[n, pl.ds(row + 1, 2 * turns, stride=stride)]
                a = jnp.where(lanes >= shift, a, b)
            if shift:
                a = pltpu.roll(a, LANES - shift, axis=1)
            framed[n, pl.ds(f, 2 * turns, stride=pitch)] = a
        return [
            jnp.concatenate(
                [framed[n, (part * turns + t) * pitch : (part * turns + t) * pitch + cycle] for t in range(turns)],
                axis=0,
            )
            for part in range(2)
        ]

    def inputs_of(s, n):
        noise, data = frames_of(s, n)
        target_ref[s] = data - noise
        level = jnp.full((1, 1), tab[STEP, s], I32).astype(F32) / 64.0
        noisy = (1.0 - level) * noise + level * data
        cond = data * (1.0 - masked_of(s))
        return jnp.concatenate([noisy, cond], axis=1).astype(BF16)

    def encode(pieces):
        hidden = dot(jnp.concatenate([inputs_of(s, n) for n, s in enumerate(pieces)], axis=0), wpad[...])
        scale = lax.rsqrt(jnp.mean(hidden * hidden, axis=1, keepdims=True) + 1e-06)
        normed = (hidden * scale * gain).astype(BF16)
        qkv = dot(normed, wcat[...]).astype(BF16)
        for n, s in enumerate(pieces):
            rows = slice(n * BLOCK, (n + 1) * BLOCK)
            hid_ref[s] = hidden[rows]
            normed_ref[s] = normed[rows]
            qkv_ref[s] = qkv[rows]

    def receive(pieces):
        for i in pieces:
            if i:
                frame_copy(i).wait_recv()
                onward(i).start()

    def settle(pieces):
        for i in pieces:
            if i:
                onward(i).wait_recv()

    near_first = [0] + order[::-1]
    rounds = [near_first[n : n + 2] for n in range(0, dp, 2)]
    if aligned:
        receive(rounds[0])
        for n, pieces in enumerate(rounds):
            if n + 1 < len(rounds):
                receive(rounds[n + 1])
            settle(pieces)
            encode(pieces)
    else:
        for pieces in rounds:
            receive(pieces)
        for pieces in rounds:
            settle(pieces)
        for n in range(0, slots, 2):
            encode([n, n + 1])

    passed = []
    for p in range(PIECES):
        for c in range(1, pairs):
            across[p * (pairs - 1) + c - 1].wait_recv()
            f = remote(full_at(c, 0, p), full_at(c, 1, p), wfsend.at[c, p], wfrecv.at[c, p], (me, mate))
            f.start()
            passed.append(f)

    window = min(LONGEST, slots)
    heads = width // HEAD_DIM
    lane = lax.broadcasted_iota(I32, (1, width), 1) // HEAD_DIM
    masks = [lane == h for h in range(heads)]

    def split(a):
        return jnp.concatenate([jnp.where(m, a, BF16(0)) for m in masks], axis=0)

    def merge(o):
        out = o[0:BLOCK]
        for h in range(1, heads):
            out = jnp.where(masks[h], o[h * BLOCK : (h + 1) * BLOCK], out)
        return out

    def window_of(s):
        begin = jnp.minimum(tab[FIRST, s], slots - window)
        at = [tab[SLOT_AT, begin + i] for i in range(window)]
        valid = [
            (begin + i >= tab[FIRST, s]) & (begin + i < tab[FIRST, s] + tab[LENGTH, s])
            for i in range(window)
        ]
        return begin, at, valid

    def query_of(s):
        return split(qkv_ref[s, :, 0:width] * BF16(HEAD_DIM**-0.5))

    def window_cols(at, j):
        return jnp.concatenate([qkv_ref[i, :, j * width : (j + 1) * width] for i in at], axis=0)

    def attend(s):
        _, at, valid = window_of(s)
        place = lax.broadcasted_iota(I32, (1, window * BLOCK), 1) // BLOCK
        bias = jnp.zeros((1, window * BLOCK), F32)
        for i in range(window):
            bias = jnp.where(place == i, jnp.where(valid[i], F32(0), F32(-1e30)), bias)
        scores = dot(query_of(s), window_cols(at, 1), NT) + bias
        e = jnp.exp(scores - jnp.max(scores, axis=1, keepdims=True))
        probs = e * (1.0 / jnp.sum(e, axis=1, keepdims=True))
        p_ref[s] = probs
        short = probs.astype(BF16)
        for i in range(window):
            pb_ref[s, i] = short[:, i * BLOCK : (i + 1) * BLOCK]
        return merge(dot(short, window_cols(at, 2))).astype(BF16)

    spots = [(a, b) for a in range(pairs - 1, -1, -1) for b in (1, 0)]
    others = spots[:-1]

    def first_slot(a, b):
        return device_at(a, b)[1] * share

    def att_copy(a, b, i):
        return remote(
            att_ref.at[a, b, i], all_ref.at[a, b, i], asend.at[a, b, i], arecv.at[a, b, i],
            device_at(pairs - a, b),
        )

    for a, b in others:
        for i in range(share):
            att_ref[a, b, i] = attend(first_slot(pairs - a, b) + i)
        for i in range(share):
            att_copy(a, b, i).start()
    for i in range(share):
        all_ref[0, 0, i] = attend(my * share + i)
    for c in beside:
        c.wait_recv()
    for f in passed:
        f.wait_recv()
    loads[5].wait()
    gain2 = gain2_ref[...].astype(F32).reshape(1, -1)
    full = jnp.concatenate([out_full[a, b] for a, b in spots], axis=0)

    def do_copy(a, b, i):
        back_a = (pairs - a) % pairs
        return remote(
            dosend.at[a, b, i], do_rel.at[back_a, b, i], dsend.at[a, b, i], drecv.at[back_a, b, i],
            device_at(a, b),
        )

    def own_rows(ref):
        return jnp.concatenate([ref[my * share + i] for i in range(share)], axis=0)

    mixed = None
    for a, b in spots[::-1]:
        if (a, b) != (0, 0):
            for i in range(share):
                att_copy(a, b, i).wait_recv()
        rows = jnp.concatenate([all_ref[a, b, i] for i in range(share)], axis=0)
        part = dot(rows, out_full[a, b]).astype(BF16).astype(F32)
        mixed = part if mixed is None else mixed + part
    masked = jnp.concatenate([masked_of(my * share + i) for i in range(share)], axis=0)
    wide = (own_rows(hid_ref) + mixed).astype(BF16).astype(F32)
    rscale = lax.rsqrt(jnp.mean(wide * wide, axis=1, keepdims=True) + 1e-06)
    normalized = wide * rscale
    velocity = dot((normalized * gain2).astype(BF16), vel_ref[...], NT)
    error = (2.0 * masked * (velocity - own_rows(target_ref)[:, 0:mel])).astype(BF16)
    scaled = dot(error, vel_ref[...]) * gain2
    back = (
        rscale * (scaled - normalized * jnp.mean(scaled * normalized, axis=1, keepdims=True))
    ).astype(BF16)
    do = dot(back, full, NT).astype(BF16)
    for n, (a, b) in enumerate(spots):
        for i in range(share):
            piece_do = do[i * BLOCK : (i + 1) * BLOCK, n * width : (n + 1) * width]
            if (a, b) == (0, 0):
                do_ref[my * share + i] = piece_do
            else:
                dosend[a, b, i] = piece_do
    for a, b in others:
        for i in range(share):
            do_copy(a, b, i).start()

    def out_term(a, b):
        return dot(jnp.concatenate([all_ref[a, b, i] for i in range(share)], axis=0), back, TN)

    def o_first(c):
        return remote(osend.at[c], onear.at[c], o1s.at[c], o1r.at[c], (me, mate))

    def o_second(c):
        return remote(osum.at[c], ofar.at[c], o2s.at[c], o2r.at[c], device_at(c, 0))

    for c in range(pairs - 1, -1, -1):
        osend[c] = out_term(c, 1).astype(BF16)
        o_first(c).start()
    for c in range(pairs):
        okeep[c] = out_term(c, 0)

    def pull(s):
        _, at, _ = window_of(s)
        probs = p_ref[s]
        dprobs = dot(split(do_ref[s]), window_cols(at, 2), NT).astype(BF16).astype(F32)
        ds = (probs * (dprobs - jnp.sum(dprobs * probs, axis=1, keepdims=True))).astype(BF16)
        for n in range(window):
            ds_ref[s, n] = ds[:, n * BLOCK : (n + 1) * BLOCK]
        dq = merge(dot(ds, window_cols(at, 1))) * (HEAD_DIM**-0.5)
        dt_ref[s, 0:width] = dq.T.astype(BF16)

    for i in range(share):
        pull(my * share + i)
    for c in range(1, pairs):
        o_first(c).wait_recv()
        osum[c] = (okeep[c] + onear[c].astype(F32)).astype(BF16)
        o_second(c).start()
    for a, b in others[::-1]:
        for i in range(share):
            do_copy((pairs - a) % pairs, b, i).wait_recv()
            do_ref[first_slot(a, b) + i] = do_rel[a, b, i]

    def pick(ref, s):
        begin, at, valid = window_of(s)
        own = jnp.clip(tab[POS, s] - begin, 0, window - 1)
        return at, jnp.concatenate(
            [jnp.where(valid[i], ref[at[i], own], BF16(0)) for i in range(window)], axis=0
        )

    def values_step(s, _):
        at, probs = pick(pb_ref, s)
        couts = jnp.concatenate([split(do_ref[i]) for i in at], axis=0)
        dv_ref[s] = dot(couts, probs, TN).astype(BF16)
        return 0

    lax.fori_loop(0, slots, values_step, 0, unroll=2)

    cols = features // dp
    flat = cols % LANES == 0

    def flipped(r):
        to = me
        for bit in range(r.bit_length()):
            if r >> bit & 1:
                to = to + (1 - 2 * lax.rem(me // 2**bit, 2)) * 2**bit
        return to

    def columns(owner):
        return pl.ds(pl.multiple_of(owner * cols, cols), cols)

    class Reduction:
        def __init__(self, refs, bits, term):
            self.keep, self.out, self.near, self.sent, self.came = refs
            self.bits, self.term = bits, term

        def pieces(self, n):
            later = [0]
            for bit in self.bits[n + 1 :][::-1]:
                later = [r | bit for r in later] + later
            return later

        def copy(self, n, r):
            r = r | self.bits[n]
            return remote(
                self.out.at[r], self.near.at[r], self.sent.at[r], self.came.at[r],
                (flipped(self.bits[n]), my),
            )

        def total(self, n, r):
            value = self.keep[r]
            for p in range(n):
                self.copy(p, r).wait_recv()
                value += self.near[r | self.bits[p]].astype(F32)
            return value

        def begin(self):
            for r in self.pieces(0):
                self.out[r | self.bits[0]] = self.term(flipped(r | self.bits[0])).astype(BF16)
                self.copy(0, r).start()

        def hold(self):
            for r in self.pieces(0):
                self.keep[r] = self.term(flipped(r))

        def stage(self, n):
            for r in self.pieces(n):
                r = r | self.bits[n]
                self.out[r] = self.total(n, r).astype(BF16)
                self.copy(n, r ^ self.bits[n]).start()

        def end(self):
            return self.total(len(self.bits), 0)

        def drain(self):
            for n in range(len(self.bits)):
                for r in self.pieces(n):
                    self.copy(n, r).wait_send()

    class Direct(Reduction):
        def second(self, r):
            return remote(
                self.out.at[r], self.near.at[r], self.sent.at[r], self.came.at[r], (flipped(r), my)
            )

        def stage(self, n):
            if n == 1:
                for r in self.far:
                    self.out[r] = self.total(1, r).astype(BF16)
                    self.second(r).start()

        @property
        def far(self):
            return [r for r in self.pieces(0) if r]

        def end(self):
            value = self.total(1, 0)
            for r in self.far:
                self.second(r).wait_recv()
                value += self.near[r].astype(F32)
            return value

        def drain(self):
            for r in self.pieces(0):
                self.copy(0, r).wait_send()
            for r in self.far:
                self.second(r).wait_send()

    def product(ref, at):
        parts = jnp.concatenate([ref[s] for s in range(slots)], axis=1)
        rows = parts.shape[0]
        if flat:
            return lambda owner: dot(
                parts,
                jnp.concatenate([normed_ref[s, :, columns(owner)] for s in range(slots)], axis=0),
            )
        normed = jnp.concatenate([normed_ref[s] for s in range(slots)], axis=0)
        for n in range(0, rows, width):
            tall_ref[:, at + n : at + n + width] = dot(parts[n : n + width], normed).T
        return lambda owner: tall_ref[columns(owner), at : at + rows]

    bits = [2**n for n in range(dp.bit_length() - 1)]
    stages = range(2, len(bits))
    values = Direct(v_refs, bits, product(dv_ref, 2 * width))
    values.begin()
    values.hold()

    for u, (a, b) in enumerate(others[::-1]):
        if u == mp // 2:
            values.stage(1)
        for i in range(share):
            pull(first_slot(a, b) + i)

    def keys_step(s, _):
        at, ds = pick(ds_ref, s)
        queries = jnp.concatenate([query_of(i) for i in at], axis=0)
        dt_ref[s, width : 2 * width] = dot(queries, ds, TN).astype(BF16)
        return 0

    lax.fori_loop(0, slots, keys_step, 0, unroll=2)

    others_of = Direct(t_refs, bits, product(dt_ref, 0))
    others_of.begin()
    o_first(0).wait_recv()
    total = okeep[0] + onear[0].astype(F32)
    for c in range(1, pairs):
        o_second(c).wait_recv()
        total += ofar[c].astype(F32)
    if flat:
        okeep[0] = total
        outs = Reduction(u_refs, bits[1:2] + bits[0:1] + bits[2:], lambda owner: okeep[0, :, columns(owner)])
    else:
        tall_ref[:, 3 * width :] = total.T
        outs = Reduction(u_refs, bits[1:2] + bits[0:1] + bits[2:], lambda owner: tall_ref[columns(owner), 3 * width :])
    outs.begin()
    others_of.hold()
    outs.hold()
    for n in range(1, len(bits)):
        others_of.stage(n)
        outs.stage(n)
    for i in range(1, dp):
        count_copy(i).wait_recv()
    inverse = 1.0 / jnp.sum(tally[...], axis=0)[0:1]
    total = values.end()
    out_ref[2] = (total.T if flat else total) * inverse
    total = others_of.end()
    for j in range(2):
        part = total[j * width : (j + 1) * width].T if flat else total[:, j * width : (j + 1) * width]
        out_ref[j] = part * inverse
    total = outs.end()
    out2_ref[...] = (total if flat else total.T) * inverse[:, 0:1]

    for i in range(1, dp):
        frame_copy(i).wait_send()
        count_copy(i).wait_send()
        onward(i).wait_send()
    for c in across + beside + passed:
        c.wait_send()
    for a, b in others:
        for i in range(share):
            att_copy(a, b, i).wait_send()
            do_copy(a, b, i).wait_send()
    for c in range(pairs):
        o_first(c).wait_send()
        if c:
            o_second(c).wait_send()
    for reduction in (values, others_of, outs):
        reduction.drain()


def finish_kernel(a_ref, b_ref, qkv_ref, o_ref):
    qkv_ref[...] = a_ref[...]
    o_ref[...] = b_ref[...]


def shards(
    dp, mp, noise_blocks, data_blocks, destination, utt_blocks, span_start, span_size, timestep,
    in_weight, norm_gain, qkv_weight, out_proj, final_gain, vel_weight,
):
    slots = noise_blocks.shape[0]
    mel = noise_blocks.shape[1] // BLOCK
    features = in_weight.shape[1]
    width = qkv_weight.shape[2]
    window = min(LONGEST, slots)
    heads = width // HEAD_DIM
    share, cols = slots // mp, features // dp
    pairs = mp // 2
    flat = cols % LANES == 0
    shapes = [(n * width, cols) if flat else (cols, n * width) for n in (2, 1, 1)]
    packed = BLOCK * mel // LANES
    part_rows = (packed + 7) // 8 * 8
    cycle = math.lcm(mel, LANES) // mel

    def array(shape, kind):
        return jax.ShapeDtypeStruct(shape, kind)

    def f32(*shape):
        return pltpu.VMEM(shape, F32)

    def bf16(*shape):
        return pltpu.VMEM(shape, BF16)

    def dma(*shape):
        return pltpu.SemaphoreType.DMA(shape)

    scratch = [
        bf16(slots, BLOCK * mel), bf16(slots, BLOCK * mel), f32(2 * part_rows * slots, LANES),
        f32(2, 2 * part_rows, LANES), f32(2, 2 * (BLOCK // cycle) * (cycle + 8), LANES),
        f32(slots, BLOCK, LANES), bf16(2 * mel, features), bf16(2 * LANES, features),
        bf16(3, features, width), bf16(features, 3 * width), bf16(width, features), bf16(mel, features),
        dma(6), f32(8 if flat else features, 4 * width),
        bf16(dp, 2, part_rows, LANES), bf16(dp, 2, part_rows, LANES), f32(dp, 8, LANES),
        pltpu.SMEM((8, slots), I32), bf16(pairs, 2, width, features),
        f32(slots, BLOCK, features), bf16(slots, BLOCK, features), bf16(slots, BLOCK, 3 * width),
        f32(slots, heads * BLOCK, window * BLOCK), bf16(slots, window, heads * BLOCK, BLOCK),
        bf16(pairs, 2, share, BLOCK, width), bf16(pairs, 2, share, BLOCK, width),
        bf16(share, BLOCK, features), bf16(pairs, 2, share, BLOCK, width),
        bf16(pairs, 2, share, BLOCK, width), bf16(slots, BLOCK, width),
        bf16(slots, window, heads * BLOCK, BLOCK), bf16(slots, 2 * width, BLOCK), bf16(slots, width, BLOCK),
        f32(pairs, width, features), bf16(pairs, width, features), bf16(pairs, width, features),
        bf16(pairs, width, features), bf16(pairs, width, features),
    ]
    for shape in shapes:
        scratch += [f32(dp, *shape)] + [bf16(dp, *shape)] * 2
    scratch += [dma(dp)] * 6 + [dma(pairs, PIECES)] * 4 + [dma(pairs, 2, share)] * 4 + [dma(pairs)] * 4
    scratch += [dma(dp)] * 6
    sums, out_sum = pl.pallas_call(
        functools.partial(step_kernel, dp, mp),
        out_shape=(f32(3, cols, width), f32(width, cols)),
        in_specs=[SMEM] * 5 + [ANY, ANY, ANY, VMEM, ANY, ANY, VMEM, ANY],
        out_specs=(VMEM, VMEM),
        scratch_shapes=scratch,
        compiler_params=params(collective_id=0, has_side_effects=True),
        name="train_step",
    )(
        destination, utt_blocks, span_start, span_size, timestep, noise_blocks, data_blocks,
        in_weight, norm_gain,
        qkv_weight.transpose(1, 0, 2), out_proj, final_gain, vel_weight.T,
    )
    grad_qkv, grad_out = pl.pallas_call(
        finish_kernel,
        out_shape=(array((3, cols, width), F32), array((width, cols), F32)),
        in_specs=[VMEM, VMEM],
        out_specs=(VMEM, VMEM),
        compiler_params=params(),
        name="finish",
    )(
        pltpu.with_memory_space_constraint(sums, pltpu.VMEM),
        pltpu.with_memory_space_constraint(out_sum, pltpu.VMEM),
    )
    return grad_qkv.transpose(1, 0, 2), grad_out


def solution(mesh):
    in_specs = (
        P("dp", None), P("dp", None), P(), P("dp", None), P("dp", None), P("dp", None),
        P("dp", None), P(), P(), P(None, None, "mp"), P("mp", None), P(), P(),
    )
    out_specs = (P("dp", None, "mp"), P("mp", "dp"))
    return jax.shard_map(
        functools.partial(shards, mesh.shape["dp"], mesh.shape["mp"]),
        mesh=mesh, in_specs=in_specs, out_specs=out_specs, check_vma=False,
    )
```

```python
import functools
import math

import jax
import jax.numpy as jnp
from jax import lax
from jax.experimental import pallas as pl
from jax.experimental.pallas import tpu as pltpu
from jax.sharding import PartitionSpec as P

HEAD_DIM = 64
BLOCK = 128
LANES = 128
LONGEST = 4
MESH = pl.DeviceIdType.MESH
VMEM = pl.BlockSpec(memory_space=pltpu.VMEM)
SMEM = pl.BlockSpec(memory_space=pltpu.SMEM)
ANY = pl.BlockSpec(memory_space=pl.ANY)
F32, BF16, I32 = jnp.float32, jnp.bfloat16, jnp.int32
NN = (((1,), (0,)), ((), ()))
NT = (((1,), (1,)), ((), ()))
TN = (((0,), (0,)), ((), ()))


def dot(a, b, dims=NN):
    return lax.dot_general(a, b, dims, preferred_element_type=F32)


def params(**kw):
    return pltpu.CompilerParams(vmem_limit_bytes=56 * 2**20, **kw)


def greet(dp, mp):
    me, my = lax.axis_index("dp"), lax.axis_index("mp")
    barrier = pltpu.get_barrier_semaphore()
    for i in range(1, dp):
        pl.semaphore_signal(
            barrier, inc=1, device_id=(lax.rem(me + i, dp), my), device_id_type=MESH
        )
    for i in range(1, mp):
        pl.semaphore_signal(
            barrier, inc=1, device_id=(me, lax.rem(my + i, mp)), device_id_type=MESH
        )
    return lambda: pl.semaphore_wait(barrier, dp - 1 + mp - 1)


def remote(src, dst, send, recv, device):
    return pltpu.make_async_remote_copy(
        src, dst, send, recv, device_id=device, device_id_type=MESH
    )


PIECES = 2
SLOT_AT, POS, SOURCE, FIRST, LENGTH, LOW, HIGH, STEP = range(8)


def step_kernel(
    dp, mp,
    dest_ref, utt_ref, start_ref, size_ref, step_ref,
    noise_hbm, data_hbm, win_hbm, gain_ref, wqkv_hbm, own_hbm, gain2_ref, vel_hbm,
    out_ref, out2_ref,
    noise_ref, data_ref, flat_ref, spread, framed, target_ref, win_ref, wpad, wqkv, wcat, own_ref, vel_ref, lsem, tall_ref,
    stage, got, tally, tab, out_full,
    hid_ref, normed_ref, qkv_ref, p_ref, pb_ref, att_ref, all_ref, back_ref,
    dosend, do_rel, do_ref, ds_ref, dt_ref, dv_ref,
    okeep, osend, onear, osum, ofar,
    *refs,
):
    t_refs, v_refs, u_refs = (refs[n * 3 : n * 3 + 3] + refs[27 + n * 2 : 29 + n * 2] for n in range(3))
    fsend, frecv, csend, crecv, hsend, hrecv = refs[9:15]
    wsend, wrecv, wfsend, wfrecv, asend, arecv, dsend, drecv, o1s, o1r, o2s, o2r = refs[15:27]
    me, my = lax.axis_index("dp"), lax.axis_index("mp")
    slots = normed_ref.shape[0]
    features = normed_ref.shape[2]
    width = own_ref.shape[0]
    mel = vel_ref.shape[0]
    packed = BLOCK * mel // LANES
    part_rows = got.shape[2]
    share = slots // mp
    pair, side = my // 2, lax.rem(my, 2)
    pairs = mp // 2
    mate = pair * 2 + 1 - side
    aligned = dp == slots

    wait = greet(dp, mp)
    loads = [
        pltpu.make_async_copy(a, b, lsem.at[n]) for n, (a, b) in enumerate((
            (noise_hbm, noise_ref), (data_hbm, data_ref), (win_hbm, win_ref), (wqkv_hbm, wqkv),
            (own_hbm, own_ref), (vel_hbm, vel_ref),
        ))
    ]
    for c in loads:
        c.start()
    owners = [dest_ref[me * slots + k] // slots for k in range(slots)]
    flat_ref[pl.ds(2 * packed * slots, (2 * part_rows - 2 * packed) * slots)] = jnp.zeros(
        ((2 * part_rows - 2 * packed) * slots, LANES), F32
    )
    loads[0].wait()
    loads[1].wait()
    for part, ref in enumerate((noise_ref, data_ref)):
        for r in range(packed):
            flat_ref[pl.ds((part * packed + r) * slots, slots)] = (
                ref[:, r * LANES : (r + 1) * LANES].astype(F32)
            )
    def fill(i):
        to = lax.rem(me + i, dp)
        pick = jnp.int32(0)
        for k in range(slots):
            pick = jnp.where(owners[k] == to, k, pick)
        for part in range(2):
            stage[i, part] = flat_ref[
                pl.ds(pick + part * part_rows * slots, part_rows, stride=slots)
            ].astype(BF16)
    count = jnp.int32(0)
    for u in range(utt_ref.shape[1]):
        low = start_ref[0, u]
        high = jnp.minimum(low + size_ref[0, u], 64)
        count += (high - low) * utt_ref[0, u] * (BLOCK // 64)
    tally[0] = jnp.full(tally.shape[1:], count, I32).astype(F32)
    def frame_copy(i):
        return remote(
            stage.at[i, side], got.at[i, side], fsend.at[i], frecv.at[i],
            (lax.rem(me + i, dp), my),
        )

    def onward(i):
        return remote(
            got.at[i, side], got.at[i, side], hsend.at[i], hrecv.at[i], (me, mate)
        )

    def count_copy(i):
        return remote(tally.at[0], tally.at[i], csend.at[i], crecv.at[i], (lax.rem(me + i, dp), my))

    order = sorted(range(1, dp), key=lambda i: -min(i, dp - i))
    fill(order[0])
    wait()
    for n, i in enumerate(order):
        frame_copy(i).start()
        fill(order[n + 1] if n + 1 < len(order) else 0)
    got[0] = stage[0]
    for i in order:
        count_copy(i).start()
    loads[4].wait()
    piece = width // PIECES

    def full_at(a, b, p):
        return out_full.at[a, b, pl.ds(p * piece, piece)]

    def device_at(a, b):
        return (me, lax.rem(pair + pairs - a, pairs) * 2 + lax.rem(side + b, 2))

    def mine(p):
        return own_ref.at[pl.ds(p * piece, piece)]

    across = [
        remote(mine(p), full_at(c, 0, p), wsend.at[c, p], wrecv.at[c, p], device_at(pairs - c, 0))
        for p in range(PIECES) for c in range(1, pairs)
    ]
    beside = [
        remote(mine(p), full_at(0, 1, p), wsend.at[0, p], wrecv.at[0, p], (me, mate))
        for p in range(PIECES)
    ]
    for c in across + beside:
        c.start()
    out_full[0, 0] = own_ref[...]

    def find(i, found):
        d = dest_ref[i]
        return tuple(jnp.where(d == me * slots + j, i // slots, o) for j, o in enumerate(found))

    origin = lax.fori_loop(0, dp * slots, find, (jnp.int32(0),) * slots)
    origin = [lax.rem(me + dp - o, dp) for o in origin]
    for s in range(slots):
        if aligned:
            tab[SLOT_AT, s] = origin[s]
            pos = jnp.int32(0)
            for j in range(slots):
                pos = jnp.where(origin[j] == s, j, pos)
        else:
            tab[SLOT_AT, s] = jnp.int32(s)
            tab[SOURCE, s] = origin[s]
            pos = jnp.int32(s)
        at = first = length = low = high = step = jnp.int32(0)
        for u in range(utt_ref.shape[1]):
            n = utt_ref[0, u]
            inside = (pos >= at) & (pos < at + n)
            first = jnp.where(inside, at, first)
            length = jnp.where(inside, n, length)
            low = jnp.where(inside, start_ref[0, u] * n * (BLOCK // 64), low)
            high = jnp.where(inside, (start_ref[0, u] + size_ref[0, u]) * n * (BLOCK // 64), high)
            step = jnp.where(inside, step_ref[0, u], step)
            at = at + n
        tab[POS, s] = pos
        tab[FIRST, s] = first
        tab[LENGTH, s] = length
        tab[LOW, s] = low
        tab[HIGH, s] = high
        tab[STEP, s] = step

    loads[2].wait()
    wpad[...] = jnp.zeros_like(wpad)
    wpad[0:mel] = win_ref[0:mel]
    wpad[LANES : LANES + mel] = win_ref[mel : 2 * mel]
    loads[3].wait()
    for j in range(3):
        wcat[:, j * width : (j + 1) * width] = wqkv[j]
    gain = gain_ref[...].astype(F32).reshape(1, -1)

    def masked_of(s):
        frame = (tab[POS, s] - tab[FIRST, s]) * BLOCK + lax.broadcasted_iota(I32, (BLOCK, 1), 0)
        return ((frame >= tab[LOW, s]) & (frame < tab[HIGH, s])).astype(F32)

    cycle = math.lcm(mel, LANES) // mel
    turns, pitch = BLOCK // cycle, cycle + 8
    stride = cycle * mel // LANES
    lanes = lax.broadcasted_iota(I32, (1, LANES), 1)

    def frames_of(s, n):
        src = s if aligned else tab[SOURCE, s]
        for part in range(2):
            spread[n, part * part_rows : (part + 1) * part_rows] = got[src, part].astype(F32)
        for f in range(cycle):
            row, shift = f * mel // LANES, f * mel % LANES
            a = spread[n, pl.ds(row, 2 * turns, stride=stride)]
            if shift + mel > LANES:
                b = spread[n, pl.ds(row + 1, 2 * turns, stride=stride)]
                a = jnp.where(lanes >= shift, a, b)
            if shift:
                a = pltpu.roll(a, LANES - shift, axis=1)
            framed[n, pl.ds(f, 2 * turns, stride=pitch)] = a
        return [
            jnp.concatenate(
                [framed[n, (part * turns + t) * pitch : (part * turns + t) * pitch + cycle] for t in range(turns)],
                axis=0,
            )
            for part in range(2)
        ]

    def inputs_of(s, n):
        noise, data = frames_of(s, n)
        target_ref[s] = data - noise
        level = jnp.full((1, 1), tab[STEP, s], I32).astype(F32) / 64.0
        noisy = (1.0 - level) * noise + level * data
        cond = data * (1.0 - masked_of(s))
        return jnp.concatenate([noisy, cond], axis=1).astype(BF16)

    def encode(pieces):
        hidden = dot(jnp.concatenate([inputs_of(s, n) for n, s in enumerate(pieces)], axis=0), wpad[...])
        scale = lax.rsqrt(jnp.mean(hidden * hidden, axis=1, keepdims=True) + 1e-06)
        normed = (hidden * scale * gain).astype(BF16)
        qkv = dot(normed, wcat[...]).astype(BF16)
        for n, s in enumerate(pieces):
            rows = slice(n * BLOCK, (n + 1) * BLOCK)
            hid_ref[s] = hidden[rows]
            normed_ref[s] = normed[rows]
            qkv_ref[s] = qkv[rows]

    def receive(pieces):
        for i in pieces:
            if i:
                frame_copy(i).wait_recv()
                onward(i).start()

    def settle(pieces):
        for i in pieces:
            if i:
                onward(i).wait_recv()

    near_first = [0] + order[::-1]
    rounds = [near_first[n : n + 2] for n in range(0, dp, 2)]
    if aligned:
        receive(rounds[0])
        for n, pieces in enumerate(rounds):
            if n + 1 < len(rounds):
                receive(rounds[n + 1])
            settle(pieces)
            encode(pieces)
    else:
        for pieces in rounds:
            receive(pieces)
        for pieces in rounds:
            settle(pieces)
        for n in range(0, slots, 2):
            encode([n, n + 1])

    passed = []
    for p in range(PIECES):
        for c in range(1, pairs):
            across[p * (pairs - 1) + c - 1].wait_recv()
            f = remote(full_at(c, 0, p), full_at(c, 1, p), wfsend.at[c, p], wfrecv.at[c, p], (me, mate))
            f.start()
            passed.append(f)

    window = min(LONGEST, slots)
    heads = width // HEAD_DIM
    lane = lax.broadcasted_iota(I32, (1, width), 1) // HEAD_DIM
    masks = [lane == h for h in range(heads)]

    def split(a):
        return jnp.concatenate([jnp.where(m, a, BF16(0)) for m in masks], axis=0)

    def merge(o):
        out = o[0:BLOCK]
        for h in range(1, heads):
            out = jnp.where(masks[h], o[h * BLOCK : (h + 1) * BLOCK], out)
        return out

    def window_of(s):
        begin = jnp.minimum(tab[FIRST, s], slots - window)
        at = [tab[SLOT_AT, begin + i] for i in range(window)]
        valid = [
            (begin + i >= tab[FIRST, s]) & (begin + i < tab[FIRST, s] + tab[LENGTH, s])
            for i in range(window)
        ]
        return begin, at, valid

    def query_of(s):
        return split(qkv_ref[s, :, 0:width] * BF16(HEAD_DIM**-0.5))

    def window_cols(at, j):
        return jnp.concatenate([qkv_ref[i, :, j * width : (j + 1) * width] for i in at], axis=0)

    def attend(s):
        _, at, valid = window_of(s)
        place = lax.broadcasted_iota(I32, (1, window * BLOCK), 1) // BLOCK
        bias = jnp.zeros((1, window * BLOCK), F32)
        for i in range(window):
            bias = jnp.where(place == i, jnp.where(valid[i], F32(0), F32(-1e30)), bias)
        scores = dot(query_of(s), window_cols(at, 1), NT) + bias
        e = jnp.exp(scores - jnp.max(scores, axis=1, keepdims=True))
        probs = e * (1.0 / jnp.sum(e, axis=1, keepdims=True))
        p_ref[s] = probs
        short = probs.astype(BF16)
        for i in range(window):
            pb_ref[s, i] = short[:, i * BLOCK : (i + 1) * BLOCK]
        return merge(dot(short, window_cols(at, 2))).astype(BF16)

    spots = [(a, b) for a in range(pairs - 1, -1, -1) for b in (1, 0)]
    others = spots[:-1]

    def first_slot(a, b):
        return device_at(a, b)[1] * share

    def att_copy(a, b, i):
        return remote(
            att_ref.at[a, b, i], all_ref.at[a, b, i], asend.at[a, b, i], arecv.at[a, b, i],
            device_at(pairs - a, b),
        )

    for a, b in others:
        for i in range(share):
            att_ref[a, b, i] = attend(first_slot(pairs - a, b) + i)
        for i in range(share):
            att_copy(a, b, i).start()
    for i in range(share):
        all_ref[0, 0, i] = attend(my * share + i)
    for c in beside:
        c.wait_recv()
    for f in passed:
        f.wait_recv()
    loads[5].wait()
    gain2 = gain2_ref[...].astype(F32).reshape(1, -1)
    full = jnp.concatenate([out_full[a, b] for a, b in spots], axis=0)

    def do_copy(a, b, i):
        back_a = (pairs - a) % pairs
        return remote(
            dosend.at[a, b, i], do_rel.at[back_a, b, i], dsend.at[a, b, i], drecv.at[back_a, b, i],
            device_at(a, b),
        )

    def own_rows(ref):
        return jnp.concatenate([ref[my * share + i] for i in range(share)], axis=0)

    mixed = None
    for a, b in spots[::-1]:
        if (a, b) != (0, 0):
            for i in range(share):
                att_copy(a, b, i).wait_recv()
        rows = jnp.concatenate([all_ref[a, b, i] for i in range(share)], axis=0)
        part = dot(rows, out_full[a, b]).astype(BF16).astype(F32)
        mixed = part if mixed is None else mixed + part
    masked = jnp.concatenate([masked_of(my * share + i) for i in range(share)], axis=0)
    wide = (own_rows(hid_ref) + mixed).astype(BF16).astype(F32)
    rscale = lax.rsqrt(jnp.mean(wide * wide, axis=1, keepdims=True) + 1e-06)
    normalized = wide * rscale
    velocity = dot((normalized * gain2).astype(BF16), vel_ref[...], NT)
    error = (2.0 * masked * (velocity - own_rows(target_ref)[:, 0:mel])).astype(BF16)
    scaled = dot(error, vel_ref[...]) * gain2
    back = (
        rscale * (scaled - normalized * jnp.mean(scaled * normalized, axis=1, keepdims=True))
    ).astype(BF16)
    do = dot(back, full, NT).astype(BF16)
    for n, (a, b) in enumerate(spots):
        for i in range(share):
            piece_do = do[i * BLOCK : (i + 1) * BLOCK, n * width : (n + 1) * width]
            if (a, b) == (0, 0):
                do_ref[my * share + i] = piece_do
            else:
                dosend[a, b, i] = piece_do
    for a, b in others:
        for i in range(share):
            do_copy(a, b, i).start()

    def out_term(a, b):
        return dot(jnp.concatenate([all_ref[a, b, i] for i in range(share)], axis=0), back, TN)

    def o_first(c):
        return remote(osend.at[c], onear.at[c], o1s.at[c], o1r.at[c], (me, mate))

    def o_second(c):
        return remote(osum.at[c], ofar.at[c], o2s.at[c], o2r.at[c], device_at(c, 0))

    for c in range(pairs - 1, -1, -1):
        osend[c] = out_term(c, 1).astype(BF16)
        o_first(c).start()
    for c in range(pairs):
        okeep[c] = out_term(c, 0)

    def pull(s):
        _, at, _ = window_of(s)
        probs = p_ref[s]
        dprobs = dot(split(do_ref[s]), window_cols(at, 2), NT).astype(BF16).astype(F32)
        ds = (probs * (dprobs - jnp.sum(dprobs * probs, axis=1, keepdims=True))).astype(BF16)
        for n in range(window):
            ds_ref[s, n] = ds[:, n * BLOCK : (n + 1) * BLOCK]
        dq = merge(dot(ds, window_cols(at, 1))) * (HEAD_DIM**-0.5)
        dt_ref[s, 0:width] = dq.T.astype(BF16)

    for i in range(share):
        pull(my * share + i)
    for c in range(1, pairs):
        o_first(c).wait_recv()
        osum[c] = (okeep[c] + onear[c].astype(F32)).astype(BF16)
        o_second(c).start()
    for a, b in others[::-1]:
        for i in range(share):
            do_copy((pairs - a) % pairs, b, i).wait_recv()
            do_ref[first_slot(a, b) + i] = do_rel[a, b, i]

    def pick(ref, s):
        begin, at, valid = window_of(s)
        own = jnp.clip(tab[POS, s] - begin, 0, window - 1)
        return at, jnp.concatenate(
            [jnp.where(valid[i], ref[at[i], own], BF16(0)) for i in range(window)], axis=0
        )

    def values_step(s, _):
        at, probs = pick(pb_ref, s)
        couts = jnp.concatenate([split(do_ref[i]) for i in at], axis=0)
        dv_ref[s] = dot(couts, probs, TN).astype(BF16)
        return 0

    lax.fori_loop(0, slots, values_step, 0, unroll=2)

    cols = features // dp
    flat = cols % LANES == 0

    def flipped(r):
        to = me
        for bit in range(r.bit_length()):
            if r >> bit & 1:
                to = to + (1 - 2 * lax.rem(me // 2**bit, 2)) * 2**bit
        return to

    def columns(owner):
        return pl.ds(pl.multiple_of(owner * cols, cols), cols)

    class Reduction:
        def __init__(self, refs, bits, term):
            self.keep, self.out, self.near, self.sent, self.came = refs
            self.bits, self.term = bits, term

        def pieces(self, n):
            later = [0]
            for bit in self.bits[n + 1 :][::-1]:
                later = [r | bit for r in later] + later
            return later

        def copy(self, n, r):
            r = r | self.bits[n]
            return remote(
                self.out.at[r], self.near.at[r], self.sent.at[r], self.came.at[r],
                (flipped(self.bits[n]), my),
            )

        def total(self, n, r):
            value = self.keep[r]
            for p in range(n):
                self.copy(p, r).wait_recv()
                value += self.near[r | self.bits[p]].astype(F32)
            return value

        def begin(self):
            for r in self.pieces(0):
                self.out[r | self.bits[0]] = self.term(flipped(r | self.bits[0])).astype(BF16)
                self.copy(0, r).start()

        def hold(self):
            for r in self.pieces(0):
                self.keep[r] = self.term(flipped(r))

        def stage(self, n):
            for r in self.pieces(n):
                r = r | self.bits[n]
                self.out[r] = self.total(n, r).astype(BF16)
                self.copy(n, r ^ self.bits[n]).start()

        def end(self):
            return self.total(len(self.bits), 0)

        def drain(self):
            for n in range(len(self.bits)):
                for r in self.pieces(n):
                    self.copy(n, r).wait_send()

    class Direct(Reduction):
        def second(self, r):
            return remote(
                self.out.at[r], self.near.at[r], self.sent.at[r], self.came.at[r], (flipped(r), my)
            )

        def stage(self, n):
            if n == 1:
                for r in self.far:
                    self.out[r] = self.total(1, r).astype(BF16)
                    self.second(r).start()

        @property
        def far(self):
            return [r for r in self.pieces(0) if r]

        def end(self):
            value = self.total(1, 0)
            for r in self.far:
                self.second(r).wait_recv()
                value += self.near[r].astype(F32)
            return value

        def drain(self):
            for r in self.pieces(0):
                self.copy(0, r).wait_send()
            for r in self.far:
                self.second(r).wait_send()

    def product(ref, at):
        parts = jnp.concatenate([ref[s] for s in range(slots)], axis=1)
        rows = parts.shape[0]
        if flat:
            return lambda owner: dot(
                parts,
                jnp.concatenate([normed_ref[s, :, columns(owner)] for s in range(slots)], axis=0),
            )
        normed = jnp.concatenate([normed_ref[s] for s in range(slots)], axis=0)
        for n in range(0, rows, width):
            tall_ref[:, at + n : at + n + width] = dot(parts[n : n + width], normed).T
        return lambda owner: tall_ref[columns(owner), at : at + rows]

    bits = [2**n for n in range(dp.bit_length() - 1)]
    stages = range(2, len(bits))
    values = Direct(v_refs, bits, product(dv_ref, 2 * width))
    values.begin()
    values.hold()

    for u, (a, b) in enumerate(others[::-1]):
        if u == mp // 2:
            values.stage(1)
        for i in range(share):
            pull(first_slot(a, b) + i)

    def keys_step(s, _):
        at, ds = pick(ds_ref, s)
        queries = jnp.concatenate([query_of(i) for i in at], axis=0)
        dt_ref[s, width : 2 * width] = dot(queries, ds, TN).astype(BF16)
        return 0

    lax.fori_loop(0, slots, keys_step, 0, unroll=2)

    others_of = Direct(t_refs, bits, product(dt_ref, 0))
    others_of.begin()
    o_first(0).wait_recv()
    total = okeep[0] + onear[0].astype(F32)
    for c in range(1, pairs):
        o_second(c).wait_recv()
        total += ofar[c].astype(F32)
    if flat:
        okeep[0] = total
        outs = Reduction(u_refs, bits[1:2] + bits[0:1] + bits[2:], lambda owner: okeep[0, :, columns(owner)])
    else:
        tall_ref[:, 3 * width :] = total.T
        outs = Reduction(u_refs, bits[1:2] + bits[0:1] + bits[2:], lambda owner: tall_ref[columns(owner), 3 * width :])
    outs.begin()
    others_of.hold()
    outs.hold()
    for n in range(1, len(bits)):
        others_of.stage(n)
        outs.stage(n)
    for i in range(1, dp):
        count_copy(i).wait_recv()
    inverse = 1.0 / jnp.sum(tally[...], axis=0)[0:1]
    total = values.end()
    out_ref[2] = (total.T if flat else total) * inverse
    total = others_of.end()
    for j in range(2):
        part = total[j * width : (j + 1) * width].T if flat else total[:, j * width : (j + 1) * width]
        out_ref[j] = part * inverse
    total = outs.end()
    out2_ref[...] = (total if flat else total.T) * inverse[:, 0:1]

    for i in range(1, dp):
        frame_copy(i).wait_send()
        count_copy(i).wait_send()
        onward(i).wait_send()
    for c in across + beside + passed:
        c.wait_send()
    for a, b in others:
        for i in range(share):
            att_copy(a, b, i).wait_send()
            do_copy(a, b, i).wait_send()
    for c in range(pairs):
        o_first(c).wait_send()
        if c:
            o_second(c).wait_send()
    for reduction in (values, others_of, outs):
        reduction.drain()


def finish_kernel(a_ref, b_ref, qkv_ref, o_ref):
    qkv_ref[...] = a_ref[...]
    o_ref[...] = b_ref[...]


def shards(
    dp, mp, noise_blocks, data_blocks, destination, utt_blocks, span_start, span_size, timestep,
    in_weight, norm_gain, qkv_weight, out_proj, final_gain, vel_weight,
):
    slots = noise_blocks.shape[0]
    mel = noise_blocks.shape[1] // BLOCK
    features = in_weight.shape[1]
    width = qkv_weight.shape[2]
    window = min(LONGEST, slots)
    heads = width // HEAD_DIM
    share, cols = slots // mp, features // dp
    pairs = mp // 2
    flat = cols % LANES == 0
    shapes = [(n * width, cols) if flat else (cols, n * width) for n in (2, 1, 1)]
    packed = BLOCK * mel // LANES
    part_rows = (packed + 7) // 8 * 8
    cycle = math.lcm(mel, LANES) // mel

    def array(shape, kind):
        return jax.ShapeDtypeStruct(shape, kind)

    def f32(*shape):
        return pltpu.VMEM(shape, F32)

    def bf16(*shape):
        return pltpu.VMEM(shape, BF16)

    def dma(*shape):
        return pltpu.SemaphoreType.DMA(shape)

    scratch = [
        bf16(slots, BLOCK * mel), bf16(slots, BLOCK * mel), f32(2 * part_rows * slots, LANES),
        f32(2, 2 * part_rows, LANES), f32(2, 2 * (BLOCK // cycle) * (cycle + 8), LANES),
        f32(slots, BLOCK, LANES), bf16(2 * mel, features), bf16(2 * LANES, features),
        bf16(3, features, width), bf16(features, 3 * width), bf16(width, features), bf16(mel, features),
        dma(6), f32(8 if flat else features, 4 * width),
        bf16(dp, 2, part_rows, LANES), bf16(dp, 2, part_rows, LANES), f32(dp, 8, LANES),
        pltpu.SMEM((8, slots), I32), bf16(pairs, 2, width, features),
        f32(slots, BLOCK, features), bf16(slots, BLOCK, features), bf16(slots, BLOCK, 3 * width),
        f32(slots, heads * BLOCK, window * BLOCK), bf16(slots, window, heads * BLOCK, BLOCK),
        bf16(pairs, 2, share, BLOCK, width), bf16(pairs, 2, share, BLOCK, width),
        bf16(share, BLOCK, features), bf16(pairs, 2, share, BLOCK, width),
        bf16(pairs, 2, share, BLOCK, width), bf16(slots, BLOCK, width),
        bf16(slots, window, heads * BLOCK, BLOCK), bf16(slots, 2 * width, BLOCK), bf16(slots, width, BLOCK),
        f32(pairs, width, features), bf16(pairs, width, features), bf16(pairs, width, features),
        bf16(pairs, width, features), bf16(pairs, width, features),
    ]
    for shape in shapes:
        scratch += [f32(dp, *shape)] + [bf16(dp, *shape)] * 2
    scratch += [dma(dp)] * 6 + [dma(pairs, PIECES)] * 4 + [dma(pairs, 2, share)] * 4 + [dma(pairs)] * 4
    scratch += [dma(dp)] * 6
    sums, out_sum = pl.pallas_call(
        functools.partial(step_kernel, dp, mp),
        out_shape=(f32(3, cols, width), f32(width, cols)),
        in_specs=[SMEM] * 5 + [ANY, ANY, ANY, VMEM, ANY, ANY, VMEM, ANY],
        out_specs=(VMEM, VMEM),
        scratch_shapes=scratch,
        compiler_params=params(collective_id=0, has_side_effects=True),
        name="train_step",
    )(
        destination, utt_blocks, span_start, span_size, timestep, noise_blocks, data_blocks,
        in_weight, norm_gain,
        qkv_weight.transpose(1, 0, 2), out_proj, final_gain, vel_weight.T,
    )
    grad_qkv, grad_out = pl.pallas_call(
        finish_kernel,
        out_shape=(array((3, cols, width), F32), array((width, cols), F32)),
        in_specs=[VMEM, VMEM],
        out_specs=(VMEM, VMEM),
        compiler_params=params(),
        name="finish",
    )(
        pltpu.with_memory_space_constraint(sums, pltpu.VMEM),
        pltpu.with_memory_space_constraint(out_sum, pltpu.VMEM),
    )
    return grad_qkv.transpose(1, 0, 2), grad_out


def solution(mesh):
    in_specs = (
        P("dp", None), P("dp", None), P(), P("dp", None), P("dp", None), P("dp", None),
        P("dp", None), P(), P(), P(None, None, "mp"), P("mp", None), P(), P(),
    )
    out_specs = (P("dp", None, "mp"), P("mp", "dp"))
    return jax.shard_map(
        functools.partial(shards, mesh.shape["dp"], mesh.shape["mp"]),
        mesh=mesh, in_specs=in_specs, out_specs=out_specs, check_vma=False,
    )
```
